512 devices in a mesh: sta: 64 (over x, z, core), tpl: 8 (over y).
Axes of the slice: x: 4, y: 8, z: 8, core: 2. Of those that a mesh axis runs over, the one named last changes fastest.
Arguments:
- waveform: bfloat16 [64, 3, 6583], P('sta'), may hold values from -150 to 150
- templates: bfloat16 [512, 64, 1536], P('tpl', 'sta'), may hold values from -6 to 6
- lags: int32 [512, 64], P('tpl', 'sta'), may hold values from 0 to 3000
- present: int32 [512, 64], P('tpl', 'sta'), may hold values 0 or 1
Outputs:
- score: float32 [3072, 512], P('sta', 'tpl')
- scale_mad: float32 [512], P('tpl')
- peak: float32 [3072], P('sta')
The draws below stay inside these ranges and needn't reach their ends.
All inputs are finite; a program needn't handle non-finite values. No bound on the sum of `present` on one device may be relied on, other than what follows from the above.
Results may differ from the reference program's by a relative error of at most 0.0003.
Values may be sent and summed in bfloat16 or wider, within the bound.
A program may use at most 64 MiB of HBM per device.

```python
import jax
import jax.numpy as jnp
from jax import lax

LEN = 512
CHANS = 3
LAG = 3000
BINS = 1024
STATIONS = 64
TEMPLATES = 512
TOUT = 3072
SAMPLES = 6583


def draw_waveform(key, part):
    key_noise = jax.random.fold_in(key, 11)
    key_scale = jax.random.fold_in(key, 12)
    timeline = jnp.arange(SAMPLES, dtype=jnp.float32) / SAMPLES
    envelope = jnp.exp(jnp.log(3.0) * timeline)
    noise = jnp.clip(jax.random.normal(key_noise, (STATIONS, 3, SAMPLES), jnp.float32), -5.0, 5.0)
    scales = jnp.exp(jax.random.uniform(key_scale, (STATIONS, 1, 1), jnp.float32, 0.0, jnp.log(10.0)))
    return (noise * scales * envelope).astype(jnp.bfloat16)


def touch_ends(drawn, own_key, smallest, top_value):
    longest = drawn.shape.index(max(drawn.shape))
    spots = []
    for shift in (0, 1):
        where = [jax.random.randint(jax.random.fold_in(own_key, axis), (), 0, length) for axis, length in enumerate(drawn.shape)]
        where[longest] = (where[longest] + shift) % drawn.shape[longest]
        spots.append(tuple(where))
    return drawn.at[spots[0]].set(smallest).at[spots[1]].set(top_value)


def shard_levels(own_key, extent, shards, least, high):
    loudness, own = 1.0, jax.random.fold_in(own_key, 6)
    for axis_at, blocks in shards:
        draws = jnp.exp(jax.random.uniform(jax.random.fold_in(own, axis_at), (blocks,), jnp.float32, least / len(shards), high / len(shards)))
        loudness = loudness * jnp.repeat(draws, extent[axis_at] // blocks).reshape([-1 if axis == axis_at else 1 for axis in range(len(extent))])
    return loudness


def normal_values(own_key, extent, scale, most, pieces=(), held_as=jnp.bfloat16):
    values = scale * jax.random.normal(own_key, extent, jnp.float32)
    if pieces:
        values = values * shard_levels(own_key, extent, pieces, -0.22, 0.18)
    return jnp.clip(values, -most, most).astype(held_as)


def setup_inputs(seed: int = 0) -> dict:
    streams_of = jax.random.split(jax.random.key(seed), 5)
    waveform = draw_waveform(jax.random.fold_in(streams_of[4], 71), 0)
    templates = normal_values(streams_of[1], (TEMPLATES, STATIONS, CHANS * LEN), 1.0, 6.0, ((0, 8), (1, 64)))
    lags = touch_ends(jax.random.randint(streams_of[2], (TEMPLATES, STATIONS), 0, LAG + 1), jax.random.fold_in(streams_of[2], 1), 0, LAG).astype(jnp.int32)
    present = touch_ends((jax.random.randint(streams_of[3], (TEMPLATES, STATIONS), 0, 4) < 3).astype(jnp.int32), jax.random.fold_in(streams_of[3], 1), 0, 1)
    return dict(waveform=waveform, templates=templates, lags=lags, present=present)


def toeplitz_rows(record, length, columns):
    count = record.shape[1]
    chans = record.shape[0]
    tiled = jnp.broadcast_to(record[:, None, :], (chans, length + 1, count))
    tiled = tiled.reshape(chans, (length + 1) * count)[:, :length * (count + 1)]
    tiled = tiled.reshape(chans, length, count + 1)[:, :, :columns]
    return tiled.reshape(chans * length, columns)

def shift_rows(block, offsets, count):
    return jax.vmap(lambda row, offset: lax.dynamic_slice_in_dim(row, offset, count))(block, offsets.astype(jnp.int32))

def hat_counts(values, nbins):
    width = 512.0 / nbins
    ncols = values.shape[1]
    position = jnp.clip(jnp.abs(values) / width - 0.5, 0.0, nbins - 1.0)
    lower = jnp.minimum(jnp.floor(position), nbins - 2.0)
    weight = position - lower
    index = lower.astype(jnp.int32) + nbins * jnp.arange(ncols, dtype=jnp.int32)[None, :]
    flat_index = index.reshape(-1)
    flat_weight = weight.reshape(-1)
    counts = jax.ops.segment_sum(1.0 - flat_weight, flat_index, num_segments=ncols * nbins)
    counts = counts + jax.ops.segment_sum(flat_weight, flat_index + 1, num_segments=ncols * nbins)
    return counts.reshape(ncols, nbins)

def median_abs(counts, halfway):
    width = 512.0 / counts.shape[1]
    running = jnp.cumsum(counts, axis=1)
    earlier = running - counts
    share = jnp.clip((halfway - earlier) / jnp.maximum(counts, 1.0), 0.0, 1.0)
    return width * lax.optimization_barrier(jnp.sum(share, axis=1))

def reference(waveform, templates, lags, present):
    total = TOUT
    span = TOUT + LAG
    tnorm = jnp.sqrt(lax.optimization_barrier(jnp.sum(templates.astype(jnp.float32) ** 2, axis=2)) + 1e-06)

    def station(stack, items):
        record, pattern, offsets, member, scaling = items
        columns = toeplitz_rows(record, LEN, span)
        corr = jnp.dot(pattern, columns, preferred_element_type=jnp.float32) / scaling[:, None]
        moved = shift_rows(corr, offsets, total) * member[:, None].astype(jnp.float32)
        return (stack + moved, None)
    start = jnp.zeros((templates.shape[0], total), jnp.float32)
    stack, unused = lax.scan(station, start, (waveform, jnp.swapaxes(templates, 0, 1), lags.T, present.T, tnorm.T))
    stack = stack.T
    counts = hat_counts(stack, BINS)
    median = median_abs(counts, 0.5 * total)
    scale_mad = 1.4826 * median
    score = stack / scale_mad[None, :]
    peak = lax.optimization_barrier(jnp.max(score, axis=1))
    return (score, scale_mad, peak)
```

```python
import functools

import jax
import jax.numpy as jnp
from jax import lax
from jax.experimental import pallas as pl
from jax.experimental.pallas import tpu as pltpu
from jax.sharding import PartitionSpec as P

LEN = 512
CHANS = 3
SAMPLES = 6583
BINS = 1024
TOUT = 3072
NT = 64
TAPS = 128
NQ = LEN // TAPS
NBLK = 52
CH = 4
ROWS = TOUT // 128
OWN = TOUT // 64
F32 = jnp.float32
BF16 = jnp.bfloat16
MESH = pl.DeviceIdType.MESH


def kernel(
    wave_ref, temp_ref, lag_ref, pres_ref, score_ref, mad_ref, peak_ref,
    wrow, amat, hank, part, scl, sendc, own, recvc, sendx, recvx, sendz, recvz,
    outr, got, pk, pkgot,
    sem_cs, sem_cr, sem_xs, sem_xr, sem_zs, sem_zr, sem_os, sem_or, sem_ps, sem_pr,
):
    s = lax.axis_index("sta")
    tp = lax.axis_index("tpl")
    x, z, c = s // 16, (s // 2) % 8, s % 2

    def dev(xx, zz, cc):
        return (xx * 16 + zz * 2 + cc, tp)

    barrier = pltpu.get_barrier_semaphore()

    def greet(i, _):
        pl.semaphore_signal(barrier, inc=1, device_id=((s + i) % 64, tp), device_id_type=MESH)
        return 0

    lax.fori_loop(1, 64, greet, 0)

    def greet_tpl(i, _):
        pl.semaphore_signal(barrier, inc=1, device_id=(s, (tp + i) % 8), device_id_type=MESH)
        return 0

    lax.fori_loop(1, 8, greet_tpl, 0)

    wrow[...] = jnp.zeros(wrow.shape, F32)
    wrow[0:CHANS, 0:SAMPLES] = wave_ref[...].astype(F32)

    total = jnp.zeros((NT, 128), F32)
    flip_i = lax.broadcasted_iota(jnp.int32, (128, 128), 0)
    flip_j = lax.broadcasted_iota(jnp.int32, (128, 128), 1)
    flip = jnp.where(flip_i + flip_j == 127, 1.0, 0.0).astype(BF16)
    for ch in range(CHANS):
        for q in range(NQ):
            piece = temp_ref[:, (ch * NQ + q) * 128 : (ch * NQ + q + 1) * 128]
            wide = piece.astype(F32)
            total = total + wide * wide
            turned = jnp.dot(piece, flip, preferred_element_type=F32).astype(BF16)
            amat[q * NT : (q + 1) * NT, ch * 128 : (ch + 1) * 128] = turned
    norm = jnp.sqrt(jnp.sum(total, axis=1, keepdims=True) + 1e-6)
    scl[...] = jnp.broadcast_to(1.0 / norm, (NT, 128))

    rho = lax.broadcasted_iota(jnp.int32, (128, 128), 0)
    lane = lax.broadcasted_iota(jnp.int32, (128, 128), 1)
    first = lane <= rho

    def chunk(j, _):
        for ch in range(CHANS):
            turned = []
            for b in range(CH + 1):
                at = pl.multiple_of((j * CH + b) * 128, 128)
                row = wrow[ch : ch + 1, pl.ds(at, 128)]
                turned.append(
                    pltpu.roll(jnp.broadcast_to(row, (128, 128)), 1, 1, stride=1, stride_axis=0)
                )
            for b in range(CH):
                block = jnp.where(first, turned[b], turned[b + 1])
                hank[ch * 128 : (ch + 1) * 128, b * 128 : (b + 1) * 128] = block.astype(BF16)
        out = jnp.dot(amat[...], hank[...], preferred_element_type=F32)
        for g in range(NQ * NT // 8):
            for b in range(CH):
                part[pl.ds(g * 8 * NBLK + j * CH + b, 8, stride=NBLK), :] = out[
                    g * 8 : (g + 1) * 8, b * 128 : (b + 1) * 128
                ]
        return 0

    lax.fori_loop(0, NBLK // CH, chunk, 0)

    lane24 = lax.broadcasted_iota(jnp.int32, (ROWS, 128), 1)

    def shifted(t):
        lag = lag_ref[0, t]
        here = pres_ref[0, t].astype(F32)
        a, r = lag // 128, lag % 128
        left = right = None
        for q in range(NQ):
            at = (q * NT + t) * NBLK + q + a
            one, two = part[pl.ds(at, ROWS), :], part[pl.ds(at + 1, ROWS), :]
            left = one if left is None else left + one
            right = two if right is None else right + two
        by = (128 - r) % 128
        left, right = pltpu.roll(left, by, 1), pltpu.roll(right, by, 1)
        return jnp.where(lane24 < 128 - r, left, right) * (scl[pl.ds(t, 1), :] * here)

    def copy_c(d):
        return pltpu.make_async_remote_copy(
            src_ref=sendc.at[d], dst_ref=recvc.at[d], send_sem=sem_cs.at[d], recv_sem=sem_cr.at[d],
            device_id=dev(x, z, 1 - c), device_id_type=MESH)

    def copy_x(d):
        return pltpu.make_async_remote_copy(
            src_ref=sendx.at[d - 1], dst_ref=recvx.at[d - 1], send_sem=sem_xs.at[d - 1],
            recv_sem=sem_xr.at[d - 1], device_id=dev((x + d) % 4, z, c), device_id_type=MESH)

    def copy_z(d):
        return pltpu.make_async_remote_copy(
            src_ref=sendz.at[d - 1], dst_ref=recvz.at[d - 1], send_sem=sem_zs.at[d - 1],
            recv_sem=sem_zr.at[d - 1], device_id=dev(x, (z + d) % 8, c), device_id_type=MESH)

    def fold(d):
        copy_c(d).wait_recv()
        if d > 0:
            sendx[d - 1] = own[d] + recvc[d]
            copy_x(d).start()

    previous = None
    for d in (2, 1, 3, 0):
        base = ((x + d) % 4) * 16

        def theirs(i, _):
            for k in range(4):
                zz = i * 4 + k
                sendc[d, zz] = shifted(base + zz * 2 + 1 - c)
            return 0

        def ours(i, _):
            for k in range(4):
                zz = i * 4 + k
                own[d, zz] = shifted(base + zz * 2 + c)
            return 0

        lax.fori_loop(0, 2, theirs, 0)
        if previous is None:
            pl.semaphore_wait(barrier, 63 + 7)
        copy_c(d).start()
        lax.fori_loop(0, 2, ours, 0)
        if previous is not None:
            fold(previous)
        previous = d
    fold(0)
    for d in (1, 3, 2):
        copy_x(d).wait_recv()

    def reduced(zz):
        return (own[0, zz] + recvc[0, zz]) + (recvx[0, zz] + recvx[1, zz] + recvx[2, zz])

    for d in (4, 3, 5, 2, 6, 1, 7):
        sendz[d - 1] = reduced((z + d) % 8)
        copy_z(d).start()
    row = reduced(z)
    for d in (1, 7, 2, 6, 3, 5, 4):
        copy_z(d).wait_recv()
        row = row + recvz[d - 1]

    pos = jnp.clip(jnp.abs(row) * (BINS / 512.0) - 0.5, 0.0, BINS - 1.0)
    low = jnp.minimum(jnp.floor(pos), BINS - 2.0)
    high = jnp.floor(low * (1.0 / 32.0))
    inside = pos - 32.0 * high
    iota_h = lax.broadcasted_iota(jnp.int32, (32, 128), 0).astype(F32)
    iota_l = lax.broadcasted_iota(jnp.int32, (40, 128), 0).astype(F32)
    ones, hats = [], [[], [], []]
    for i in range(ROWS):
        ones.append(jnp.where(iota_h == high[i : i + 1, :], 1.0, 0.0).astype(BF16))
        hat = jnp.maximum(1.0 - jnp.abs(inside[i : i + 1, :] - iota_l), 0.0)
        for k in range(3):
            near = hat.astype(BF16)
            hats[k].append(near)
            hat = hat - near.astype(F32)
    ones = jnp.concatenate(ones, axis=1)
    counts = None
    for k in range(3):
        got_k = lax.dot_general(
            jnp.concatenate(hats[k], axis=1), ones, (((1,), (1,)), ((), ())),
            preferred_element_type=F32)
        counts = got_k if counts is None else counts + got_k
    over = jnp.concatenate([jnp.zeros((1, 1), F32), counts[32:33, 0:31]], axis=1)
    row_l = lax.broadcasted_iota(jnp.int32, (32, 32), 0)
    col_h = lax.broadcasted_iota(jnp.int32, (32, 32), 1)
    counts = counts[0:32, :] + jnp.where(row_l == 0, jnp.broadcast_to(over, (32, 32)), 0.0)
    below = jnp.where(col_h < row_l, 1.0, 0.0)
    above = jnp.where(row_l < col_h, 1.0, 0.0)
    sums = jnp.broadcast_to(jnp.sum(counts, axis=0, keepdims=True), (8, 32))
    before = jnp.dot(below, counts, precision=lax.Precision.HIGHEST, preferred_element_type=F32)
    before = before + jnp.dot(
        sums, above, precision=lax.Precision.HIGHEST, preferred_element_type=F32)[0:1, :]
    share = jnp.clip((0.5 * TOUT - before) / jnp.maximum(counts, 1.0), 0.0, 1.0)
    share = jnp.sum(jnp.sum(share, axis=1, keepdims=True), axis=0, keepdims=True)
    mad = 1.4826 * ((512.0 / BINS) * share)
    pk[...] = row / mad
    madrow = jnp.broadcast_to(mad, (8, 128))

    lane8 = lax.broadcasted_iota(jnp.int32, (8, 128), 1)
    for j in range(8):
        at, off = (OWN * j) // 128, (OWN * j) % 128
        piece = pk[pl.ds(at, 8, stride=3), :]
        if off:
            piece = pltpu.roll(piece, 128 - off, 1)
            if off + OWN > 128:
                nxt = pltpu.roll(pk[pl.ds(at + 1, 8, stride=3), :], 128 - off, 1)
                piece = jnp.where(lane8 < 128 - off, piece, nxt)
        piece = jnp.where(lane8 < OWN, piece, madrow)
        for g in range(8):
            outr[8 * g + j] = piece[g : g + 1, :]

    def copy_o(i):
        to = (s + i) % 64
        return pltpu.make_async_remote_copy(
            src_ref=outr.at[to], dst_ref=got.at[s], send_sem=sem_os, recv_sem=sem_or,
            device_id=(to, tp), device_id_type=MESH)

    def send(i, _):
        copy_o((i + 32) % 64).start()
        return 0

    lax.fori_loop(0, 32, send, 0)
    lax.fori_loop(33, 64, send, 0)
    got[s] = outr[s]
    pltpu.make_async_copy(outr.at[pl.ds(0, 63)], got.at[pl.ds(0, 63)], sem_or).wait()

    best = jnp.max(got[...], axis=0)
    pkgot[0] = best

    def copy_p(d):
        return pltpu.make_async_remote_copy(
            src_ref=pkgot.at[0], dst_ref=pkgot.at[d], send_sem=sem_ps.at[d - 1],
            recv_sem=sem_pr.at[d - 1], device_id=(s, (tp + d) % 8), device_id_type=MESH)

    for d in (4, 3, 5, 2, 6, 1, 7):
        copy_p(d).start()
    flat = jnp.concatenate([got[i] for i in range(64)] + [jnp.zeros((64, 128), F32)], axis=0)
    turned = flat.T
    score_ref[...] = turned[0:OWN, 0:NT]
    mad_ref[...] = turned[OWN : OWN + 1, 0:NT]
    for d in (1, 7, 2, 6, 3, 5, 4):
        copy_p(d).wait_recv()
        best = jnp.maximum(best, pkgot[d])
    peak_ref[...] = best[:, 0:OWN]

    for d in range(4):
        copy_c(d).wait_send()
    for d in range(1, 4):
        copy_x(d).wait_send()
    for d in range(1, 8):
        copy_z(d).wait_send()
        copy_p(d).wait_send()
    pltpu.make_async_copy(outr.at[pl.ds(0, 63)], got.at[pl.ds(0, 63)], sem_os).wait()


def on_device(waveform, templates, lags, present):
    vmem = pl.BlockSpec(memory_space=pltpu.VMEM)
    smem = pl.BlockSpec(memory_space=pltpu.SMEM)
    dma = pltpu.SemaphoreType.DMA
    score, mad, peak = pl.pallas_call(
        kernel,
        out_shape=(
            jax.ShapeDtypeStruct((OWN, NT), F32),
            jax.ShapeDtypeStruct((1, NT), F32),
            jax.ShapeDtypeStruct((1, OWN), F32),
        ),
        in_specs=[vmem, vmem, smem, smem],
        out_specs=(vmem, vmem, vmem),
        scratch_shapes=[
            pltpu.VMEM((8, (NBLK + 1) * 128), F32),
            pltpu.VMEM((NQ * NT, CHANS * TAPS), BF16),
            pltpu.VMEM((CHANS * TAPS, CH * 128), BF16),
            pltpu.VMEM((NQ * NT * NBLK, 128), F32),
            pltpu.VMEM((NT, 128), F32),
            pltpu.VMEM((4, 8, ROWS, 128), F32),
            pltpu.VMEM((4, 8, ROWS, 128), F32),
            pltpu.VMEM((4, 8, ROWS, 128), F32),
            pltpu.VMEM((3, 8, ROWS, 128), F32),
            pltpu.VMEM((3, 8, ROWS, 128), F32),
            pltpu.VMEM((7, ROWS, 128), F32),
            pltpu.VMEM((7, ROWS, 128), F32),
            pltpu.VMEM((64, 1, 128), F32),
            pltpu.VMEM((64, 1, 128), F32),
            pltpu.VMEM((ROWS, 128), F32),
            pltpu.VMEM((8, 1, 128), F32),
            dma((4,)), dma((4,)), dma((3,)), dma((3,)), dma((7,)), dma((7,)),
            dma(()), dma(()), dma((7,)), dma((7,)),
        ],
        compiler_params=pltpu.CompilerParams(
            collective_id=0, has_side_effects=True, vmem_limit_bytes=50 * 1024 * 1024),
    )(waveform[0], templates[:, 0, :], lags.reshape(1, NT), present.reshape(1, NT))
    return score, mad[0], peak[0]


def solution(mesh):
    return jax.shard_map(
        on_device,
        mesh=mesh,
        in_specs=(P("sta", None, None), P("tpl", "sta", None), P("tpl", "sta"), P("tpl", "sta")),
        out_specs=(P("sta", "tpl"), P("tpl"), P("sta")),
        check_vma=False,
    )
```

```python
import functools

import jax
import jax.numpy as jnp
from jax import lax
from jax.experimental import pallas as pl
from jax.experimental.pallas import tpu as pltpu
from jax.sharding import PartitionSpec as P

LEN = 512
CHANS = 3
SAMPLES = 6583
BINS = 1024
TOUT = 3072
NT = 64
TAPS = 128
NQ = LEN // TAPS
NBLK = 52
CH = 4
ROWS = TOUT // 128
OWN = TOUT // 64
F32 = jnp.float32
BF16 = jnp.bfloat16
MESH = pl.DeviceIdType.MESH


def kernel(
    wave_hbm, temp_hbm, lag_hbm, pres_hbm, score_ref, mad_ref, peak_ref,
    wave_ref, temp_ref, lag_ref, pres_ref, sem_in, wrow, amat, hank, hank2, part, scl, sendc, own, recvc, sendx, recvx, sendz, recvz,
    outr, got, pk, pkgot,
    sem_cs, sem_cr, sem_xs, sem_xr, sem_zs, sem_zr, sem_os, sem_or, sem_ps, sem_pr,
):
    s = lax.axis_index("sta")
    tp = lax.axis_index("tpl")
    x, z, c = s // 16, (s // 2) % 8, s % 2

    def dev(xx, zz, cc):
        return (xx * 16 + zz * 2 + cc, tp)

    inputs = [
        pltpu.make_async_copy(a, b, sem_in.at[i])
        for i, (a, b) in enumerate(
            ((temp_hbm, temp_ref), (wave_hbm, wave_ref), (lag_hbm, lag_ref), (pres_hbm, pres_ref))
        )
    ]
    for copy in inputs:
        copy.start()

    barrier = pltpu.get_barrier_semaphore()
    for i in range(1, 8):
        pl.semaphore_signal(barrier, inc=1, device_id=(s, (tp + i) % 8), device_id_type=MESH)

    def greet(i):
        pl.semaphore_signal(barrier, inc=1, device_id=((s + i) % 64, tp), device_id_type=MESH)

    wrow[...] = jnp.zeros(wrow.shape, F32)
    for copy in inputs:
        copy.wait()
    wrow[0:CHANS, 0:SAMPLES] = wave_ref[...].astype(F32)

    total = jnp.zeros((NT, 128), F32)
    flip_i = lax.broadcasted_iota(jnp.int32, (128, 128), 0)
    flip_j = lax.broadcasted_iota(jnp.int32, (128, 128), 1)
    flip = jnp.where(flip_i + flip_j == 127, 1.0, 0.0).astype(BF16)
    for ch in range(CHANS):
        for q in range(NQ):
            piece = temp_ref[:, (ch * NQ + q) * 128 : (ch * NQ + q + 1) * 128]
            wide = piece.astype(F32)
            total = total + wide * wide
            turned = jnp.dot(piece, flip, preferred_element_type=F32).astype(BF16)
            amat[q * NT : (q + 1) * NT, ch * 128 : (ch + 1) * 128] = turned
    norm = jnp.sqrt(jnp.sum(total, axis=1, keepdims=True) + 1e-6)
    scl[...] = jnp.broadcast_to(1.0 / norm, (NT, 128))

    rho = lax.broadcasted_iota(jnp.int32, (128, 128), 0)
    lane = lax.broadcasted_iota(jnp.int32, (128, 128), 1)
    first = lane <= rho

    def build(j, into):
        for ch in range(CHANS):
            turned = []
            for b in range(CH + 1):
                at = pl.multiple_of((j * CH + b) * 128, 128)
                row = wrow[ch : ch + 1, pl.ds(at, 128)]
                turned.append(
                    pltpu.roll(jnp.broadcast_to(row, (128, 128)), 1, 1, stride=1, stride_axis=0)
                )
            for b in range(CH):
                block = jnp.where(first, turned[b], turned[b + 1])
                into[ch * 128 : (ch + 1) * 128, b * 128 : (b + 1) * 128] = block.astype(BF16)

    def multiply(j, held):
        out = jnp.dot(amat[...], held[...], preferred_element_type=F32)
        for g in range(NQ * NT // 8):
            for b in range(CH):
                part[pl.ds(g * 8 * NBLK + j * CH + b, 8, stride=NBLK), :] = out[
                    g * 8 : (g + 1) * 8, b * 128 : (b + 1) * 128
                ]

    def chunks(i, _):
        for k in range(10):
            greet(1 + i * 10 + k)
        multiply(2 * i, hank)
        build(2 * i + 1, hank2)
        multiply(2 * i + 1, hank2)
        build(2 * i + 2, hank)
        return 0

    for i in range(61, 64):
        greet(i)
    build(0, hank)
    lax.fori_loop(0, NBLK // CH // 2, chunks, 0)
    multiply(NBLK // CH - 1, hank)

    lane24 = lax.broadcasted_iota(jnp.int32, (ROWS, 128), 1)

    def shifted(t):
        lag = lag_ref[0, t]
        here = pres_ref[0, t].astype(F32)
        a, r = lag // 128, lag % 128
        left = right = None
        for q in range(NQ):
            at = (q * NT + t) * NBLK + q + a
            one, two = part[pl.ds(at, ROWS), :], part[pl.ds(at + 1, ROWS), :]
            left = one if left is None else left + one
            right = two if right is None else right + two
        by = (128 - r) % 128
        left, right = pltpu.roll(left, by, 1), pltpu.roll(right, by, 1)
        return jnp.where(lane24 < 128 - r, left, right) * (scl[pl.ds(t, 1), :] * here)

    def copy_c(d):
        return pltpu.make_async_remote_copy(
            src_ref=sendc.at[d], dst_ref=recvc.at[d], send_sem=sem_cs.at[d], recv_sem=sem_cr.at[d],
            device_id=dev(x, z, 1 - c), device_id_type=MESH)

    def copy_x(d):
        return pltpu.make_async_remote_copy(
            src_ref=sendx.at[d - 1], dst_ref=recvx.at[d - 1], send_sem=sem_xs.at[d - 1],
            recv_sem=sem_xr.at[d - 1], device_id=dev((x + d) % 4, z, c), device_id_type=MESH)

    def copy_z(d):
        return pltpu.make_async_remote_copy(
            src_ref=sendz.at[d - 1], dst_ref=recvz.at[d - 1], send_sem=sem_zs.at[d - 1],
            recv_sem=sem_zr.at[d - 1], device_id=dev(x, (z + d) % 8, c), device_id_type=MESH)

    def fold(d):
        copy_c(d).wait_recv()
        if d > 0:
            sendx[d - 1] = own[d] + recvc[d]
            copy_x(d).start()

    previous = None
    for d in (2, 1, 3, 0):
        base = ((x + d) % 4) * 16

        def theirs(i, _):
            for k in range(4):
                zz = i * 4 + k
                sendc[d, zz] = shifted(base + zz * 2 + 1 - c)
            return 0

        def ours(i, _):
            for k in range(4):
                zz = i * 4 + k
                own[d, zz] = shifted(base + zz * 2 + c)
            return 0

        lax.fori_loop(0, 2, theirs, 0)
        if previous is None:
            pl.semaphore_wait(barrier, 63 + 7)
        copy_c(d).start()
        lax.fori_loop(0, 2, ours, 0)
        if previous is not None:
            fold(previous)
        previous = d
    fold(0)
    for d in (1, 3, 2):
        copy_x(d).wait_recv()

    def reduced(zz):
        return (own[0, zz] + recvc[0, zz]) + (recvx[0, zz] + recvx[1, zz] + recvx[2, zz])

    for d in (4, 3, 5, 2, 6, 1, 7):
        sendz[d - 1] = reduced((z + d) % 8)
        copy_z(d).start()
    row = reduced(z)
    for d in (1, 7, 2, 6, 3, 5, 4):
        copy_z(d).wait_recv()
        row = row + recvz[d - 1]

    pos = jnp.clip(jnp.abs(row) * (BINS / 512.0) - 0.5, 0.0, BINS - 1.0)
    low = jnp.minimum(jnp.floor(pos), BINS - 2.0)
    high = jnp.floor(low * (1.0 / 32.0))
    inside = pos - 32.0 * high
    iota_h = lax.broadcasted_iota(jnp.int32, (32, 128), 0).astype(F32)
    iota_l = lax.broadcasted_iota(jnp.int32, (40, 128), 0).astype(F32)
    ones, hats = [], [[], [], []]
    for i in range(ROWS):
        ones.append(jnp.where(iota_h == high[i : i + 1, :], 1.0, 0.0).astype(BF16))
        hat = jnp.maximum(1.0 - jnp.abs(inside[i : i + 1, :] - iota_l), 0.0)
        for k in range(3):
            near = hat.astype(BF16)
            hats[k].append(near)
            hat = hat - near.astype(F32)
    ones = jnp.concatenate(ones, axis=1)
    counts = None
    for k in range(3):
        got_k = lax.dot_general(
            jnp.concatenate(hats[k], axis=1), ones, (((1,), (1,)), ((), ())),
            preferred_element_type=F32)
        counts = got_k if counts is None else counts + got_k
    over = jnp.concatenate([jnp.zeros((1, 1), F32), counts[32:33, 0:31]], axis=1)
    row_l = lax.broadcasted_iota(jnp.int32, (32, 32), 0)
    col_h = lax.broadcasted_iota(jnp.int32, (32, 32), 1)
    counts = counts[0:32, :] + jnp.where(row_l == 0, jnp.broadcast_to(over, (32, 32)), 0.0)
    below = jnp.where(col_h < row_l, 1.0, 0.0)
    above = jnp.where(row_l < col_h, 1.0, 0.0)
    sums = jnp.broadcast_to(jnp.sum(counts, axis=0, keepdims=True), (8, 32))
    before = jnp.dot(below, counts, precision=lax.Precision.HIGHEST, preferred_element_type=F32)
    before = before + jnp.dot(
        sums, above, precision=lax.Precision.HIGHEST, preferred_element_type=F32)[0:1, :]
    share = jnp.clip((0.5 * TOUT - before) / jnp.maximum(counts, 1.0), 0.0, 1.0)
    share = jnp.sum(jnp.sum(share, axis=1, keepdims=True), axis=0, keepdims=True)
    mad = 1.4826 * ((512.0 / BINS) * share)
    pk[...] = row / mad
    madrow = jnp.broadcast_to(mad, (8, 128))

    lane8 = lax.broadcasted_iota(jnp.int32, (8, 128), 1)
    for j in range(8):
        at, off = (OWN * j) // 128, (OWN * j) % 128
        piece = pk[pl.ds(at, 8, stride=3), :]
        if off:
            piece = pltpu.roll(piece, 128 - off, 1)
            if off + OWN > 128:
                nxt = pltpu.roll(pk[pl.ds(at + 1, 8, stride=3), :], 128 - off, 1)
                piece = jnp.where(lane8 < 128 - off, piece, nxt)
        piece = jnp.where(lane8 < OWN, piece, madrow)
        for g in range(8):
            outr[8 * g + j] = piece[g : g + 1, :]

    def copy_o(i):
        to = (s + i) % 64
        return pltpu.make_async_remote_copy(
            src_ref=outr.at[to], dst_ref=got.at[s], send_sem=sem_os, recv_sem=sem_or,
            device_id=(to, tp), device_id_type=MESH)

    def send(i, _):
        copy_o((i + 32) % 64).start()
        return 0

    lax.fori_loop(0, 32, send, 0)
    lax.fori_loop(33, 64, send, 0)
    got[s] = outr[s]
    pltpu.make_async_copy(outr.at[pl.ds(0, 63)], got.at[pl.ds(0, 63)], sem_or).wait()

    best = jnp.max(got[...], axis=0)
    pkgot[0] = best

    def copy_p(d):
        return pltpu.make_async_remote_copy(
            src_ref=pkgot.at[0], dst_ref=pkgot.at[d], send_sem=sem_ps.at[d - 1],
            recv_sem=sem_pr.at[d - 1], device_id=(s, (tp + d) % 8), device_id_type=MESH)

    for d in (4, 3, 5, 2, 6, 1, 7):
        copy_p(d).start()
    flat = jnp.concatenate([got[i] for i in range(64)] + [jnp.zeros((64, 128), F32)], axis=0)
    turned = flat.T
    score_ref[...] = turned[0:OWN, 0:NT]
    mad_ref[...] = turned[OWN : OWN + 1, 0:NT]
    for d in (1, 7, 2, 6, 3, 5, 4):
        copy_p(d).wait_recv()
        best = jnp.maximum(best, pkgot[d])
    peak_ref[...] = best[:, 0:OWN]

    for d in range(4):
        copy_c(d).wait_send()
    for d in range(1, 4):
        copy_x(d).wait_send()
    for d in range(1, 8):
        copy_z(d).wait_send()
        copy_p(d).wait_send()
    pltpu.make_async_copy(outr.at[pl.ds(0, 63)], got.at[pl.ds(0, 63)], sem_os).wait()


def put_out(a, b, c, a_out, b_out, c_out, sems):
    copies = [
        pltpu.make_async_copy(one, two, sems.at[i])
        for i, (one, two) in enumerate(((a, a_out), (b, b_out), (c, c_out)))
    ]
    for copy in copies:
        copy.start()
    for copy in copies:
        copy.wait()


def on_device(waveform, templates, lags, present):
    vmem = pl.BlockSpec(memory_space=pltpu.VMEM)
    dma = pltpu.SemaphoreType.DMA
    hbm = pl.BlockSpec(memory_space=pltpu.HBM)
    results = pl.pallas_call(
        kernel,
        out_shape=(
            jax.ShapeDtypeStruct((OWN, NT), F32),
            jax.ShapeDtypeStruct((1, NT), F32),
            jax.ShapeDtypeStruct((1, OWN), F32),
        ),
        in_specs=[hbm, hbm, hbm, hbm],
        out_specs=(vmem, vmem, vmem),
        scratch_shapes=[
            pltpu.VMEM((CHANS, SAMPLES), BF16),
            pltpu.VMEM((NT, CHANS * LEN), BF16),
            pltpu.SMEM((1, NT), jnp.int32),
            pltpu.SMEM((1, NT), jnp.int32),
            dma((4,)),
            pltpu.VMEM((8, (NBLK + 1) * 128), F32),
            pltpu.VMEM((NQ * NT, CHANS * TAPS), BF16),
            pltpu.VMEM((CHANS * TAPS, CH * 128), BF16),
            pltpu.VMEM((CHANS * TAPS, CH * 128), BF16),
            pltpu.VMEM((NQ * NT * NBLK, 128), F32),
            pltpu.VMEM((NT, 128), F32),
            pltpu.VMEM((4, 8, ROWS, 128), F32),
            pltpu.VMEM((4, 8, ROWS, 128), F32),
            pltpu.VMEM((4, 8, ROWS, 128), F32),
            pltpu.VMEM((3, 8, ROWS, 128), F32),
            pltpu.VMEM((3, 8, ROWS, 128), F32),
            pltpu.VMEM((7, ROWS, 128), F32),
            pltpu.VMEM((7, ROWS, 128), F32),
            pltpu.VMEM((64, 1, 128), F32),
            pltpu.VMEM((64, 1, 128), F32),
            pltpu.VMEM((ROWS, 128), F32),
            pltpu.VMEM((8, 1, 128), F32),
            dma((4,)), dma((4,)), dma((3,)), dma((3,)), dma((7,)), dma((7,)),
            dma(()), dma(()), dma((7,)), dma((7,)),
        ],
        compiler_params=pltpu.CompilerParams(
            collective_id=0, has_side_effects=True, vmem_limit_bytes=56500000),
    )(waveform[0], templates[:, 0, :], lags.reshape(1, NT), present.reshape(1, NT))
    score, mad, peak = pl.pallas_call(
        put_out,
        out_shape=(
            jax.ShapeDtypeStruct((OWN, NT), F32),
            jax.ShapeDtypeStruct((1, NT), F32),
            jax.ShapeDtypeStruct((1, OWN), F32),
        ),
        in_specs=[vmem, vmem, vmem],
        out_specs=(hbm, hbm, hbm),
        scratch_shapes=[dma((3,))],
        compiler_params=pltpu.CompilerParams(vmem_limit_bytes=1024 * 1024),
    )(*results)
    return score, mad[0], peak[0]


def solution(mesh):
    return jax.shard_map(
        on_device,
        mesh=mesh,
        in_specs=(P("sta", None, None), P("tpl", "sta", None), P("tpl", "sta"), P("tpl", "sta")),
        out_specs=(P("sta", "tpl"), P("tpl"), P("sta")),
        check_vma=False,
    )
```

```python
import functools

import jax
import jax.numpy as jnp
from jax import lax
from jax.experimental import pallas as pl
from jax.experimental.pallas import tpu as pltpu
from jax.sharding import PartitionSpec as P

LEN = 512
CHANS = 3
SAMPLES = 6583
BINS = 1024
TOUT = 3072
NT = 64
TAPS = 128
NQ = LEN // TAPS
NBLK = 52
CH = 4
ROWS = TOUT // 128
OWN = TOUT // 64
F32 = jnp.float32
BF16 = jnp.bfloat16
MESH = pl.DeviceIdType.MESH
AWAY = (4, 3, 5, 2, 6, 1, 7, 0)


def kernel(
    wave_hbm, temp_hbm, lag_hbm, pres_hbm, score_ref, mad_ref, peak_ref,
    wave_ref, temp_ref, lag_ref, pres_ref, sem_in, wrow, amat, hank, hank2, part, scl, sendc, own, recvc, sendx, recvx, sendz, recvz,
    outr, got, pk, pkgot,
    sem_cs, sem_cr, sem_xs, sem_xr, sem_zs, sem_zr, sem_os, sem_or, sem_ps, sem_pr,
):
    s = lax.axis_index("sta")
    tp = lax.axis_index("tpl")
    x, z, c = s // 16, (s // 2) % 8, s % 2

    def dev(xx, zz, cc):
        return (xx * 16 + zz * 2 + cc, tp)

    inputs = [
        pltpu.make_async_copy(a, b, sem_in.at[i])
        for i, (a, b) in enumerate(
            ((temp_hbm, temp_ref), (wave_hbm, wave_ref), (lag_hbm, lag_ref), (pres_hbm, pres_ref))
        )
    ]
    for copy in inputs:
        copy.start()

    barrier = pltpu.get_barrier_semaphore()
    for i in range(1, 8):
        pl.semaphore_signal(barrier, inc=1, device_id=(s, (tp + i) % 8), device_id_type=MESH)
        pl.semaphore_signal(barrier, inc=1, device_id=dev(x, (z + i) % 8, c), device_id_type=MESH)
    for i in range(1, 4):
        pl.semaphore_signal(barrier, inc=1, device_id=dev((x + i) % 4, z, c), device_id_type=MESH)
    pl.semaphore_signal(barrier, inc=1, device_id=dev(x, z, 1 - c), device_id_type=MESH)

    wrow[...] = jnp.zeros(wrow.shape, F32)
    for copy in inputs:
        copy.wait()
    wrow[0:CHANS, 0:SAMPLES] = wave_ref[...].astype(F32)

    total = jnp.zeros((NT, 128), F32)
    flip_i = lax.broadcasted_iota(jnp.int32, (128, 128), 0)
    flip_j = lax.broadcasted_iota(jnp.int32, (128, 128), 1)
    flip = jnp.where(flip_i + flip_j == 127, 1.0, 0.0).astype(BF16)
    for ch in range(CHANS):
        for q in range(NQ):
            piece = temp_ref[:, (ch * NQ + q) * 128 : (ch * NQ + q + 1) * 128]
            wide = piece.astype(F32)
            total = total + wide * wide
            turned = jnp.dot(piece, flip, preferred_element_type=F32).astype(BF16)
            amat[q * NT : (q + 1) * NT, ch * 128 : (ch + 1) * 128] = turned
    norm = jnp.sqrt(jnp.sum(total, axis=1, keepdims=True) + 1e-6)
    scl[...] = jnp.broadcast_to(1.0 / norm, (NT, 128))

    rho = lax.broadcasted_iota(jnp.int32, (128, 128), 0)
    lane = lax.broadcasted_iota(jnp.int32, (128, 128), 1)
    first = lane <= rho

    def build(j, into):
        for ch in range(CHANS):
            turned = []
            for b in range(CH + 1):
                at = pl.multiple_of((j * CH + b) * 128, 128)
                row = wrow[ch : ch + 1, pl.ds(at, 128)]
                turned.append(
                    pltpu.roll(jnp.broadcast_to(row, (128, 128)), 1, 1, stride=1, stride_axis=0)
                )
            for b in range(CH):
                block = jnp.where(first, turned[b], turned[b + 1])
                into[ch * 128 : (ch + 1) * 128, b * 128 : (b + 1) * 128] = block.astype(BF16)

    def multiply(j, held):
        out = jnp.dot(amat[...], held[...], preferred_element_type=F32)
        for g in range(NQ * NT // 8):
            for b in range(CH):
                part[pl.ds(g * 8 * NBLK + j * CH + b, 8, stride=NBLK), :] = out[
                    g * 8 : (g + 1) * 8, b * 128 : (b + 1) * 128
                ]

    def chunks(i, _):
        multiply(2 * i, hank)
        build(2 * i + 1, hank2)
        multiply(2 * i + 1, hank2)
        build(2 * i + 2, hank)
        return 0

    build(0, hank)
    lax.fori_loop(0, NBLK // CH // 2, chunks, 0)
    multiply(NBLK // CH - 1, hank)

    lane24 = lax.broadcasted_iota(jnp.int32, (ROWS, 128), 1)

    def shifted(t):
        lag = lag_ref[0, t]
        here = pres_ref[0, t].astype(F32)
        a, r = lag // 128, lag % 128
        left = right = None
        for q in range(NQ):
            at = (q * NT + t) * NBLK + q + a
            one, two = part[pl.ds(at, ROWS), :], part[pl.ds(at + 1, ROWS), :]
            left = one if left is None else left + one
            right = two if right is None else right + two
        by = (128 - r) % 128
        left, right = pltpu.roll(left, by, 1), pltpu.roll(right, by, 1)
        return jnp.where(lane24 < 128 - r, left, right) * (scl[pl.ds(t, 1), :] * here)

    def place(k):
        return (z + 4 + k // 2 - (k % 2) * k + 8) % 8

    def copy_c(k):
        return pltpu.make_async_remote_copy(
            src_ref=sendc.at[k], dst_ref=recvc.at[k], send_sem=sem_cs.at[k], recv_sem=sem_cr.at[k],
            device_id=dev(x, z, 1 - c), device_id_type=MESH)

    def copy_x(k, d):
        return pltpu.make_async_remote_copy(
            src_ref=sendx.at[k, d - 1], dst_ref=recvx.at[k, d - 1],
            send_sem=sem_xs.at[k, d - 1], recv_sem=sem_xr.at[k, d - 1],
            device_id=dev((x + d) % 4, z, c), device_id_type=MESH)

    def copy_z(k):
        return pltpu.make_async_remote_copy(
            src_ref=sendz.at[k], dst_ref=recvz.at[k], send_sem=sem_zs.at[k], recv_sem=sem_zr.at[k],
            device_id=dev(x, (z + AWAY[k]) % 8, c), device_id_type=MESH)

    def theirs(k, _):
        for d in range(4):
            sendc[k, d] = shifted(((x + d) % 4) * 16 + place(k) * 2 + 1 - c)
        copy_c(k).start()
        return 0

    def ours(k, _):
        for d in range(4):
            own[k, d] = shifted(((x + d) % 4) * 16 + place(k) * 2 + c)
        return 0

    pl.semaphore_wait(barrier, 1 + 3 + 7 + 7)
    lax.fori_loop(0, 8, theirs, 0)
    lax.fori_loop(0, 8, ours, 0)
    for k in range(8):
        copy_c(k).wait_recv()
        for d in (2, 1, 3):
            sendx[k, d - 1] = own[k, d] + recvc[k, d]
            copy_x(k, d).start()
    row = None
    for k in range(8):
        for d in (1, 3, 2):
            copy_x(k, d).wait_recv()
        row = (own[k, 0] + recvc[k, 0]) + (recvx[k, 0] + recvx[k, 1] + recvx[k, 2])
        if k < 7:
            sendz[k] = row
            copy_z(k).start()
    for k in range(7):
        copy_z(k).wait_recv()
        row = row + recvz[k]

    pos = jnp.clip(jnp.abs(row) * (BINS / 512.0) - 0.5, 0.0, BINS - 1.0)
    low = jnp.minimum(jnp.floor(pos), BINS - 2.0)
    high = jnp.floor(low * (1.0 / 32.0))
    inside = pos - 32.0 * high
    iota_h = lax.broadcasted_iota(jnp.int32, (32, 128), 0).astype(F32)
    iota_l = lax.broadcasted_iota(jnp.int32, (40, 128), 0).astype(F32)
    ones, hats = [], [[], [], []]
    for i in range(ROWS):
        ones.append(jnp.where(iota_h == high[i : i + 1, :], 1.0, 0.0).astype(BF16))
        hat = jnp.maximum(1.0 - jnp.abs(inside[i : i + 1, :] - iota_l), 0.0)
        for k in range(3):
            near = hat.astype(BF16)
            hats[k].append(near)
            hat = hat - near.astype(F32)
    ones = jnp.concatenate(ones, axis=1)
    counts = None
    for k in range(3):
        got_k = lax.dot_general(
            jnp.concatenate(hats[k], axis=1), ones, (((1,), (1,)), ((), ())),
            preferred_element_type=F32)
        counts = got_k if counts is None else counts + got_k
    over = jnp.concatenate([jnp.zeros((1, 1), F32), counts[32:33, 0:31]], axis=1)
    row_l = lax.broadcasted_iota(jnp.int32, (32, 32), 0)
    col_h = lax.broadcasted_iota(jnp.int32, (32, 32), 1)
    counts = counts[0:32, :] + jnp.where(row_l == 0, jnp.broadcast_to(over, (32, 32)), 0.0)
    below = jnp.where(col_h < row_l, 1.0, 0.0)
    above = jnp.where(row_l < col_h, 1.0, 0.0)
    sums = jnp.broadcast_to(jnp.sum(counts, axis=0, keepdims=True), (8, 32))
    before = jnp.dot(below, counts, precision=lax.Precision.HIGHEST, preferred_element_type=F32)
    before = before + jnp.dot(
        sums, above, precision=lax.Precision.HIGHEST, preferred_element_type=F32)[0:1, :]
    share = jnp.clip((0.5 * TOUT - before) / jnp.maximum(counts, 1.0), 0.0, 1.0)
    share = jnp.sum(jnp.sum(share, axis=1, keepdims=True), axis=0, keepdims=True)
    mad = 1.4826 * ((512.0 / BINS) * share)
    pk[...] = row / mad
    madrow = jnp.broadcast_to(mad, (8, 128))

    lane8 = lax.broadcasted_iota(jnp.int32, (8, 128), 1)
    for j in range(8):
        at, off = (OWN * j) // 128, (OWN * j) % 128
        piece = pk[pl.ds(at, 8, stride=3), :]
        if off:
            piece = pltpu.roll(piece, 128 - off, 1)
            if off + OWN > 128:
                nxt = pltpu.roll(pk[pl.ds(at + 1, 8, stride=3), :], 128 - off, 1)
                piece = jnp.where(lane8 < 128 - off, piece, nxt)
        piece = jnp.where(lane8 < OWN, piece, madrow)
        for g in range(8):
            outr[8 * g + j] = piece[g : g + 1, :]

    def copy_o(xx, zz, cc):
        to = xx * 16 + zz * 2 + cc
        return pltpu.make_async_remote_copy(
            src_ref=outr.at[to], dst_ref=got.at[s], send_sem=sem_os, recv_sem=sem_or,
            device_id=(to, tp), device_id_type=MESH)

    others = [(x + d) % 4 for d in range(4)]

    def send(k, _):
        zz = place(k)
        for d in (2, 1, 3, 0):
            copy_o(others[d], zz, c).start()
            copy_o(others[d], zz, 1 - c).start()
        return 0

    lax.fori_loop(0, 7, send, 0)
    for d in (2, 1, 3):
        copy_o(others[d], z, c).start()
        copy_o(others[d], z, 1 - c).start()
    copy_o(x, z, 1 - c).start()
    got[s] = outr[s]
    pltpu.make_async_copy(outr.at[pl.ds(0, 63)], got.at[pl.ds(0, 63)], sem_or).wait()

    best = jnp.max(got[...], axis=0)
    pkgot[0] = best

    def copy_p(d):
        return pltpu.make_async_remote_copy(
            src_ref=pkgot.at[0], dst_ref=pkgot.at[d], send_sem=sem_ps.at[d - 1],
            recv_sem=sem_pr.at[d - 1], device_id=(s, (tp + d) % 8), device_id_type=MESH)

    for d in (4, 3, 5, 2, 6, 1, 7):
        copy_p(d).start()
    flat = jnp.concatenate([got[i] for i in range(64)] + [jnp.zeros((64, 128), F32)], axis=0)
    turned = flat.T
    score_ref[...] = turned[0:OWN, 0:NT]
    mad_ref[...] = turned[OWN : OWN + 1, 0:NT]
    for d in (1, 7, 2, 6, 3, 5, 4):
        copy_p(d).wait_recv()
        best = jnp.maximum(best, pkgot[d])
    peak_ref[...] = best[:, 0:OWN]

    for k in range(8):
        copy_c(k).wait_send()
        for d in range(1, 4):
            copy_x(k, d).wait_send()
    for k in range(7):
        copy_z(k).wait_send()
        copy_p(k + 1).wait_send()
    pltpu.make_async_copy(outr.at[pl.ds(0, 63)], got.at[pl.ds(0, 63)], sem_os).wait()


def put_out(a, b, c, a_out, b_out, c_out, sems):
    copies = [
        pltpu.make_async_copy(one, two, sems.at[i])
        for i, (one, two) in enumerate(((a, a_out), (b, b_out), (c, c_out)))
    ]
    for copy in copies:
        copy.start()
    for copy in copies:
        copy.wait()


def on_device(waveform, templates, lags, present):
    vmem = pl.BlockSpec(memory_space=pltpu.VMEM)
    dma = pltpu.SemaphoreType.DMA
    hbm = pl.BlockSpec(memory_space=pltpu.HBM)
    results = pl.pallas_call(
        kernel,
        out_shape=(
            jax.ShapeDtypeStruct((OWN, NT), F32),
            jax.ShapeDtypeStruct((1, NT), F32),
            jax.ShapeDtypeStruct((1, OWN), F32),
        ),
        in_specs=[hbm, hbm, hbm, hbm],
        out_specs=(vmem, vmem, vmem),
        scratch_shapes=[
            pltpu.VMEM((CHANS, SAMPLES), BF16),
            pltpu.VMEM((NT, CHANS * LEN), BF16),
            pltpu.SMEM((1, NT), jnp.int32),
            pltpu.SMEM((1, NT), jnp.int32),
            dma((4,)),
            pltpu.VMEM((8, (NBLK + 1) * 128), F32),
            pltpu.VMEM((NQ * NT, CHANS * TAPS), BF16),
            pltpu.VMEM((CHANS * TAPS, CH * 128), BF16),
            pltpu.VMEM((CHANS * TAPS, CH * 128), BF16),
            pltpu.VMEM((NQ * NT * NBLK, 128), F32),
            pltpu.VMEM((NT, 128), F32),
            pltpu.VMEM((8, 4, ROWS, 128), F32),
            pltpu.VMEM((8, 4, ROWS, 128), F32),
            pltpu.VMEM((8, 4, ROWS, 128), F32),
            pltpu.VMEM((8, 3, ROWS, 128), F32),
            pltpu.VMEM((8, 3, ROWS, 128), F32),
            pltpu.VMEM((7, ROWS, 128), F32),
            pltpu.VMEM((7, ROWS, 128), F32),
            pltpu.VMEM((64, 1, 128), F32),
            pltpu.VMEM((64, 1, 128), F32),
            pltpu.VMEM((ROWS, 128), F32),
            pltpu.VMEM((8, 1, 128), F32),
            dma((8,)), dma((8,)), dma((8, 3)), dma((8, 3)), dma((7,)), dma((7,)),
            dma(()), dma(()), dma((7,)), dma((7,)),
        ],
        compiler_params=pltpu.CompilerParams(
            collective_id=0, has_side_effects=True, vmem_limit_bytes=56500000),
    )(waveform[0], templates[:, 0, :], lags.reshape(1, NT), present.reshape(1, NT))
    score, mad, peak = pl.pallas_call(
        put_out,
        out_shape=(
            jax.ShapeDtypeStruct((OWN, NT), F32),
            jax.ShapeDtypeStruct((1, NT), F32),
            jax.ShapeDtypeStruct((1, OWN), F32),
        ),
        in_specs=[vmem, vmem, vmem],
        out_specs=(hbm, hbm, hbm),
        scratch_shapes=[dma((3,))],
        compiler_params=pltpu.CompilerParams(vmem_limit_bytes=1024 * 1024),
    )(*results)
    return score, mad[0], peak[0]


def solution(mesh):
    return jax.shard_map(
        on_device,
        mesh=mesh,
        in_specs=(P("sta", None, None), P("tpl", "sta", None), P("tpl", "sta"), P("tpl", "sta")),
        out_specs=(P("sta", "tpl"), P("tpl"), P("sta")),
        check_vma=False,
    )
```

```python
import functools

import jax
import jax.numpy as jnp
from jax import lax
from jax.experimental import pallas as pl
from jax.experimental.pallas import tpu as pltpu
from jax.sharding import PartitionSpec as P

LEN = 512
CHANS = 3
SAMPLES = 6583
BINS = 1024
TOUT = 3072
NT = 64
TAPS = 128
NQ = LEN // TAPS
NBLK = 52
CH = 4
ROWS = TOUT // 128
OWN = TOUT // 64
F32 = jnp.float32
BF16 = jnp.bfloat16
MESH = pl.DeviceIdType.MESH
AWAY = (4, 3, 5, 2, 6, 1, 7, 0)


def kernel(
    wave_hbm, temp_hbm, lag_hbm, pres_hbm, score_ref, mad_ref, peak_ref,
    wave_ref, temp_ref, lag_ref, pres_ref, sem_in, wrow, amat, hank, hank2, part, scl, sendc, own, recvc, sendx, recvx, sendz, recvz,
    outr, got, pk, pkgot,
    sem_cs, sem_cr, sem_xs, sem_xr, sem_zs, sem_zr, sem_os, sem_or, sem_ps, sem_pr,
):
    s = lax.axis_index("sta")
    tp = lax.axis_index("tpl")
    x, z, c = s // 16, (s // 2) % 8, s % 2

    def dev(xx, zz, cc):
        return (xx * 16 + zz * 2 + cc, tp)

    inputs = [
        pltpu.make_async_copy(a, b, sem_in.at[i])
        for i, (a, b) in enumerate(
            ((temp_hbm, temp_ref), (wave_hbm, wave_ref), (lag_hbm, lag_ref), (pres_hbm, pres_ref))
        )
    ]
    for copy in inputs:
        copy.start()

    barrier = pltpu.get_barrier_semaphore()
    for i in range(1, 8):
        pl.semaphore_signal(barrier, inc=1, device_id=(s, (tp + i) % 8), device_id_type=MESH)
        pl.semaphore_signal(barrier, inc=1, device_id=dev(x, (z + i) % 8, c), device_id_type=MESH)
    for i in range(1, 4):
        pl.semaphore_signal(barrier, inc=1, device_id=dev((x + i) % 4, z, c), device_id_type=MESH)
    pl.semaphore_signal(barrier, inc=1, device_id=dev(x, z, 1 - c), device_id_type=MESH)

    def place(k):
        return (z + 4 + k // 2 - (k % 2) * k + 8) % 8

    spot = lax.broadcasted_iota(jnp.int32, (NT, NT), 0)
    column = lax.broadcasted_iota(jnp.int32, (NT, NT), 1)
    step, turn, mine = spot >> 3, (spot >> 1) & 3, spot & 1
    source = (((x + turn) & 3) * 16 + ((z + 4 + (step >> 1) - (step & 1) * step + 8) & 7) * 2
              + (c + 1 - mine) % 2)
    order = jnp.where(source == column, 1.0, 0.0).astype(BF16)
    flip_i = lax.broadcasted_iota(jnp.int32, (128, 128), 0)
    flip_j = lax.broadcasted_iota(jnp.int32, (128, 128), 1)
    flip = jnp.where(flip_i + flip_j == 127, 1.0, 0.0).astype(BF16)

    wrow[...] = jnp.zeros(wrow.shape, F32)
    for copy in inputs:
        copy.wait()
    wrow[0:CHANS, 0:SAMPLES] = wave_ref[...].astype(F32)

    total = jnp.zeros((NT, 128), F32)
    for ch in range(CHANS):
        for q in range(NQ):
            wide = jnp.dot(
                order, temp_ref[:, (ch * NQ + q) * 128 : (ch * NQ + q + 1) * 128],
                preferred_element_type=F32)
            total = total + wide * wide
            turned = jnp.dot(wide.astype(BF16), flip, preferred_element_type=F32).astype(BF16)
            for half in range(2):
                amat[half, q * 32 : (q + 1) * 32, ch * 128 : (ch + 1) * 128] = turned[
                    half * 32 : (half + 1) * 32, :
                ]
    norm = jnp.sqrt(jnp.sum(total, axis=1, keepdims=True) + 1e-6)
    scl[...] = jnp.broadcast_to(1.0 / norm, (NT, 128))

    rho = lax.broadcasted_iota(jnp.int32, (16, 128), 0)
    lane16 = lax.broadcasted_iota(jnp.int32, (16, 128), 1)

    def build(j, into, slot):
        for ch in range(CHANS):
            for g in range(TAPS // 16):
                first = lane16 <= rho + 16 * g
                before = None
                for b in range(CH + 1):
                    at = pl.multiple_of((j * CH + b) * 128, 128)
                    row = jnp.broadcast_to(wrow[ch : ch + 1, pl.ds(at, 128)], (16, 128))
                    after = pltpu.roll(row, 1 + 16 * g, 1, stride=1, stride_axis=0)
                    if b:
                        into[
                            slot,
                            ch * TAPS + g * 16 : ch * TAPS + (g + 1) * 16,
                            (b - 1) * 128 : b * 128,
                        ] = jnp.where(first, before, after).astype(BF16)
                    before = after

    def multiply(half, j, held, slot):
        out = jnp.dot(amat[half], held[slot], preferred_element_type=F32)
        for g in range(NQ * 4):
            for b in range(CH):
                part[pl.ds((half * NQ * 4 + g) * 8 * NBLK + j * CH + b, 8, stride=NBLK), :] = out[
                    g * 8 : (g + 1) * 8, b * 128 : (b + 1) * 128
                ]

    def first_half(i, _):
        multiply(0, 2 * i, hank, i)
        build(2 * i + 1, hank2, i)
        multiply(0, 2 * i + 1, hank2, i)
        build(2 * i + 2, hank, i + 1)
        return 0

    def second_half(i, _):
        multiply(1, 2 * i, hank, i)
        multiply(1, 2 * i + 1, hank2, i)
        return 0

    lane24 = lax.broadcasted_iota(jnp.int32, (ROWS, 128), 1)

    def shifted(k, d, mine):
        t = ((x + d) % 4) * 16 + place(k) * 2 + (c if mine else 1 - c)
        lag = lag_ref[0, t]
        here = pres_ref[0, t].astype(F32)
        a, r = lag // 128, lag % 128
        left = right = None
        for q in range(NQ):
            at = ((k // 4) * NQ * 32 + q * 32 + (k % 4) * 8 + 2 * d + mine) * NBLK + q + a
            one, two = part[pl.ds(at, ROWS), :], part[pl.ds(at + 1, ROWS), :]
            left = one if left is None else left + one
            right = two if right is None else right + two
        by = (128 - r) % 128
        left, right = pltpu.roll(left, by, 1), pltpu.roll(right, by, 1)
        scale = scl[pl.ds(k * 8 + 2 * d + mine, 1), :] * here
        return jnp.where(lane24 < 128 - r, left, right) * scale

    def copy_c(k):
        return pltpu.make_async_remote_copy(
            src_ref=sendc.at[k], dst_ref=recvc.at[k], send_sem=sem_cs.at[k], recv_sem=sem_cr.at[k],
            device_id=dev(x, z, 1 - c), device_id_type=MESH)

    def copy_x(k, d):
        return pltpu.make_async_remote_copy(
            src_ref=sendx.at[k, d - 1], dst_ref=recvx.at[k, d - 1],
            send_sem=sem_xs.at[k, d - 1], recv_sem=sem_xr.at[k, d - 1],
            device_id=dev((x + d) % 4, z, c), device_id_type=MESH)

    def copy_z(k):
        return pltpu.make_async_remote_copy(
            src_ref=sendz.at[k], dst_ref=recvz.at[k], send_sem=sem_zs.at[k], recv_sem=sem_zr.at[k],
            device_id=dev(x, (z + AWAY[k]) % 8, c), device_id_type=MESH)

    def theirs(k, _):
        for d in range(4):
            sendc[k, d] = shifted(k, d, 0)
        copy_c(k).start()
        return 0

    def ours(k, _):
        for d in range(4):
            own[k, d] = shifted(k, d, 1)
        return 0

    def fold(k):
        copy_c(k).wait_recv()
        for d in (2, 1, 3):
            sendx[k, d - 1] = own[k, d] + recvc[k, d]
            copy_x(k, d).start()

    build(0, hank, 0)
    lax.fori_loop(0, NBLK // CH // 2, first_half, 0)
    multiply(0, NBLK // CH - 1, hank, NBLK // CH // 2)
    pl.semaphore_wait(barrier, 1 + 3 + 7 + 7)
    lax.fori_loop(0, 4, theirs, 0)
    lax.fori_loop(0, 4, ours, 0)
    lax.fori_loop(0, 4, second_half, 0)
    for k in range(4):
        fold(k)
    lax.fori_loop(4, NBLK // CH // 2, second_half, 0)
    multiply(1, NBLK // CH - 1, hank, NBLK // CH // 2)
    lax.fori_loop(4, 8, theirs, 0)
    lax.fori_loop(4, 8, ours, 0)
    for k in range(4, 8):
        fold(k)
    row = None
    for k in range(8):
        for d in (1, 3, 2):
            copy_x(k, d).wait_recv()
        row = (own[k, 0] + recvc[k, 0]) + (recvx[k, 0] + recvx[k, 1] + recvx[k, 2])
        if k < 7:
            sendz[k] = row
            copy_z(k).start()
    for k in range(7):
        copy_z(k).wait_recv()
        row = row + recvz[k]

    pos = jnp.clip(jnp.abs(row) * (BINS / 512.0) - 0.5, 0.0, BINS - 1.0)
    low = jnp.minimum(jnp.floor(pos), BINS - 2.0)
    high = jnp.floor(low * (1.0 / 32.0))
    inside = pos - 32.0 * high
    iota_h = lax.broadcasted_iota(jnp.int32, (32, 128), 0).astype(F32)
    iota_l = lax.broadcasted_iota(jnp.int32, (40, 128), 0).astype(F32)
    ones, hats = [], [[], [], []]
    for i in range(ROWS):
        ones.append(jnp.where(iota_h == high[i : i + 1, :], 1.0, 0.0).astype(BF16))
        hat = jnp.maximum(1.0 - jnp.abs(inside[i : i + 1, :] - iota_l), 0.0)
        for k in range(3):
            near = hat.astype(BF16)
            hats[k].append(near)
            hat = hat - near.astype(F32)
    ones = jnp.concatenate(ones, axis=1)
    counts = None
    for k in range(3):
        got_k = lax.dot_general(
            jnp.concatenate(hats[k], axis=1), ones, (((1,), (1,)), ((), ())),
            preferred_element_type=F32)
        counts = got_k if counts is None else counts + got_k
    over = jnp.concatenate([jnp.zeros((1, 1), F32), counts[32:33, 0:31]], axis=1)
    row_l = lax.broadcasted_iota(jnp.int32, (32, 32), 0)
    col_h = lax.broadcasted_iota(jnp.int32, (32, 32), 1)
    counts = counts[0:32, :] + jnp.where(row_l == 0, jnp.broadcast_to(over, (32, 32)), 0.0)
    below = jnp.where(col_h < row_l, 1.0, 0.0)
    above = jnp.where(row_l < col_h, 1.0, 0.0)
    sums = jnp.broadcast_to(jnp.sum(counts, axis=0, keepdims=True), (8, 32))
    before = jnp.dot(below, counts, precision=lax.Precision.HIGHEST, preferred_element_type=F32)
    before = before + jnp.dot(
        sums, above, precision=lax.Precision.HIGHEST, preferred_element_type=F32)[0:1, :]
    share = jnp.clip((0.5 * TOUT - before) / jnp.maximum(counts, 1.0), 0.0, 1.0)
    share = jnp.sum(jnp.sum(share, axis=1, keepdims=True), axis=0, keepdims=True)
    mad = 1.4826 * ((512.0 / BINS) * share)
    pk[...] = row / mad
    madrow = jnp.broadcast_to(mad, (8, 128))

    lane8 = lax.broadcasted_iota(jnp.int32, (8, 128), 1)
    for j in range(8):
        at, off = (OWN * j) // 128, (OWN * j) % 128
        piece = pk[pl.ds(at, 8, stride=3), :]
        if off:
            piece = pltpu.roll(piece, 128 - off, 1)
            if off + OWN > 128:
                nxt = pltpu.roll(pk[pl.ds(at + 1, 8, stride=3), :], 128 - off, 1)
                piece = jnp.where(lane8 < 128 - off, piece, nxt)
        piece = jnp.where(lane8 < OWN, piece, madrow)
        for g in range(8):
            outr[8 * g + j] = piece[g : g + 1, :]

    def copy_o(xx, zz, cc):
        to = xx * 16 + zz * 2 + cc
        return pltpu.make_async_remote_copy(
            src_ref=outr.at[to], dst_ref=got.at[s], send_sem=sem_os, recv_sem=sem_or,
            device_id=(to, tp), device_id_type=MESH)

    others = [(x + d) % 4 for d in range(4)]

    def send(k, _):
        zz = place(k)
        for d in (2, 1, 3, 0):
            copy_o(others[d], zz, c).start()
            copy_o(others[d], zz, 1 - c).start()
        return 0

    lax.fori_loop(0, 7, send, 0)
    for d in (2, 1, 3):
        copy_o(others[d], z, c).start()
        copy_o(others[d], z, 1 - c).start()
    copy_o(x, z, 1 - c).start()
    got[s] = outr[s]
    pltpu.make_async_copy(outr.at[pl.ds(0, 63)], got.at[pl.ds(0, 63)], sem_or).wait()

    best = jnp.max(got[...], axis=0)
    pkgot[0] = best

    def copy_p(d):
        return pltpu.make_async_remote_copy(
            src_ref=pkgot.at[0], dst_ref=pkgot.at[d], send_sem=sem_ps.at[d - 1],
            recv_sem=sem_pr.at[d - 1], device_id=(s, (tp + d) % 8), device_id_type=MESH)

    for d in (4, 3, 5, 2, 6, 1, 7):
        copy_p(d).start()
    flat = jnp.concatenate([got[i] for i in range(64)] + [jnp.zeros((64, 128), F32)], axis=0)
    turned = flat.T
    score_ref[...] = turned[0:OWN, 0:NT]
    mad_ref[...] = turned[OWN : OWN + 1, 0:NT]
    for d in (1, 7, 2, 6, 3, 5, 4):
        copy_p(d).wait_recv()
        best = jnp.maximum(best, pkgot[d])
    peak_ref[...] = best[:, 0:OWN]

    for k in range(8):
        copy_c(k).wait_send()
        for d in range(1, 4):
            copy_x(k, d).wait_send()
    for k in range(7):
        copy_z(k).wait_send()
        copy_p(k + 1).wait_send()
    pltpu.make_async_copy(outr.at[pl.ds(0, 63)], got.at[pl.ds(0, 63)], sem_os).wait()


def put_out(a, b, c, a_out, b_out, c_out, sems):
    copies = [
        pltpu.make_async_copy(one, two, sems.at[i])
        for i, (one, two) in enumerate(((a, a_out), (b, b_out), (c, c_out)))
    ]
    for copy in copies:
        copy.start()
    for copy in copies:
        copy.wait()


def on_device(waveform, templates, lags, present):
    vmem = pl.BlockSpec(memory_space=pltpu.VMEM)
    dma = pltpu.SemaphoreType.DMA
    hbm = pl.BlockSpec(memory_space=pltpu.HBM)
    results = pl.pallas_call(
        kernel,
        out_shape=(
            jax.ShapeDtypeStruct((OWN, NT), F32),
            jax.ShapeDtypeStruct((1, NT), F32),
            jax.ShapeDtypeStruct((1, OWN), F32),
        ),
        in_specs=[hbm, hbm, hbm, hbm],
        out_specs=(vmem, vmem, vmem),
        scratch_shapes=[
            pltpu.VMEM((CHANS, SAMPLES), BF16),
            pltpu.VMEM((NT, CHANS * LEN), BF16),
            pltpu.SMEM((1, NT), jnp.int32),
            pltpu.SMEM((1, NT), jnp.int32),
            dma((4,)),
            pltpu.VMEM((8, (NBLK + 1) * 128), F32),
            pltpu.VMEM((2, NQ * 32, CHANS * TAPS), BF16),
            pltpu.VMEM((NBLK // CH // 2 + 1, CHANS * TAPS, CH * 128), BF16),
            pltpu.VMEM((NBLK // CH // 2, CHANS * TAPS, CH * 128), BF16),
            pltpu.VMEM((NQ * NT * NBLK, 128), F32),
            pltpu.VMEM((NT, 128), F32),
            pltpu.VMEM((8, 4, ROWS, 128), F32),
            pltpu.VMEM((8, 4, ROWS, 128), F32),
            pltpu.VMEM((8, 4, ROWS, 128), F32),
            pltpu.VMEM((8, 3, ROWS, 128), F32),
            pltpu.VMEM((8, 3, ROWS, 128), F32),
            pltpu.VMEM((7, ROWS, 128), F32),
            pltpu.VMEM((7, ROWS, 128), F32),
            pltpu.VMEM((64, 1, 128), F32),
            pltpu.VMEM((64, 1, 128), F32),
            pltpu.VMEM((ROWS, 128), F32),
            pltpu.VMEM((8, 1, 128), F32),
            dma((8,)), dma((8,)), dma((8, 3)), dma((8, 3)), dma((7,)), dma((7,)),
            dma(()), dma(()), dma((7,)), dma((7,)),
        ],
        compiler_params=pltpu.CompilerParams(
            collective_id=0, has_side_effects=True, vmem_limit_bytes=56500000),
    )(waveform[0], templates[:, 0, :], lags.reshape(1, NT), present.reshape(1, NT))
    score, mad, peak = pl.pallas_call(
        put_out,
        out_shape=(
            jax.ShapeDtypeStruct((OWN, NT), F32),
            jax.ShapeDtypeStruct((1, NT), F32),
            jax.ShapeDtypeStruct((1, OWN), F32),
        ),
        in_specs=[vmem, vmem, vmem],
        out_specs=(hbm, hbm, hbm),
        scratch_shapes=[dma((3,))],
        compiler_params=pltpu.CompilerParams(vmem_limit_bytes=1024 * 1024),
    )(*results)
    return score, mad[0], peak[0]


def solution(mesh):
    return jax.shard_map(
        on_device,
        mesh=mesh,
        in_specs=(P("sta", None, None), P("tpl", "sta", None), P("tpl", "sta"), P("tpl", "sta")),
        out_specs=(P("sta", "tpl"), P("tpl"), P("sta")),
        check_vma=False,
    )
```

```python
import functools

import jax
import jax.numpy as jnp
from jax import lax
from jax.experimental import pallas as pl
from jax.experimental.pallas import tpu as pltpu
from jax.sharding import PartitionSpec as P

LEN = 512
CHANS = 3
SAMPLES = 6583
BINS = 1024
TOUT = 3072
NT = 64
TAPS = 128
NQ = LEN // TAPS
NBLK = 52
CH = 4
ROWS = TOUT // 128
OWN = TOUT // 64
F32 = jnp.float32
BF16 = jnp.bfloat16
MESH = pl.DeviceIdType.MESH
AWAY = (4, 3, 5, 2, 6, 1, 7, 0)


def kernel(
    wave_hbm, temp_hbm, lag_hbm, pres_hbm, score_ref, mad_ref, peak_ref,
    wave_ref, temp_ref, lag_ref, pres_ref, sem_in, wrow, amat, hank, hank2, part, scl, sendc, own, recvc, sendx, recvx, sendz, recvz,
    outr, got, pk, pkgot,
    sem_cs, sem_cr, sem_xs, sem_xr, sem_zs, sem_zr, sem_os, sem_or, sem_ps, sem_pr,
):
    s = lax.axis_index("sta")
    tp = lax.axis_index("tpl")
    x, z, c = s // 16, (s // 2) % 8, s % 2

    def dev(xx, zz, cc):
        return (xx * 16 + zz * 2 + cc, tp)

    inputs = [
        pltpu.make_async_copy(a, b, sem_in.at[i])
        for i, (a, b) in enumerate(
            ((temp_hbm, temp_ref), (wave_hbm, wave_ref), (lag_hbm, lag_ref), (pres_hbm, pres_ref))
        )
    ]
    for copy in inputs:
        copy.start()

    barrier = pltpu.get_barrier_semaphore()
    for i in range(1, 8):
        pl.semaphore_signal(barrier, inc=1, device_id=(s, (tp + i) % 8), device_id_type=MESH)
        pl.semaphore_signal(barrier, inc=1, device_id=dev(x, (z + i) % 8, c), device_id_type=MESH)
    for i in range(1, 4):
        pl.semaphore_signal(barrier, inc=1, device_id=dev((x + i) % 4, z, c), device_id_type=MESH)
    pl.semaphore_signal(barrier, inc=1, device_id=dev(x, z, 1 - c), device_id_type=MESH)

    wrow[...] = jnp.zeros(wrow.shape, F32)
    for copy in inputs:
        copy.wait()
    wrow[0:CHANS, 0:SAMPLES] = wave_ref[...].astype(F32)

    total = jnp.zeros((NT, 128), F32)
    flip_i = lax.broadcasted_iota(jnp.int32, (128, 128), 0)
    flip_j = lax.broadcasted_iota(jnp.int32, (128, 128), 1)
    flip = jnp.where(flip_i + flip_j == 127, 1.0, 0.0).astype(BF16)
    for ch in range(CHANS):
        for q in range(NQ):
            piece = temp_ref[:, (ch * NQ + q) * 128 : (ch * NQ + q + 1) * 128]
            wide = piece.astype(F32)
            total = total + wide * wide
            turned = jnp.dot(piece, flip, preferred_element_type=F32).astype(BF16)
            amat[q * NT : (q + 1) * NT, ch * 128 : (ch + 1) * 128] = turned
    norm = jnp.sqrt(jnp.sum(total, axis=1, keepdims=True) + 1e-6)
    scl[...] = jnp.broadcast_to(1.0 / norm, (NT, 128))

    rho = lax.broadcasted_iota(jnp.int32, (16, 128), 0)
    lane16 = lax.broadcasted_iota(jnp.int32, (16, 128), 1)

    def build(j, into):
        for ch in range(CHANS):
            for g in range(TAPS // 16):
                first = lane16 <= rho + 16 * g
                before = None
                for b in range(CH + 1):
                    at = pl.multiple_of((j * CH + b) * 128, 128)
                    row = jnp.broadcast_to(wrow[ch : ch + 1, pl.ds(at, 128)], (16, 128))
                    after = pltpu.roll(row, 1 + 16 * g, 1, stride=1, stride_axis=0)
                    if b:
                        into[
                            ch * TAPS + g * 16 : ch * TAPS + (g + 1) * 16,
                            (b - 1) * 128 : b * 128,
                        ] = jnp.where(first, before, after).astype(BF16)
                    before = after

    def multiply(j, held):
        out = jnp.dot(amat[...], held[...], preferred_element_type=F32)
        for g in range(NQ * NT // 8):
            for b in range(CH):
                part[pl.ds(g * 8 * NBLK + j * CH + b, 8, stride=NBLK), :] = out[
                    g * 8 : (g + 1) * 8, b * 128 : (b + 1) * 128
                ]

    def chunks(i, _):
        multiply(2 * i, hank)
        build(2 * i + 1, hank2)
        multiply(2 * i + 1, hank2)
        build(2 * i + 2, hank)
        return 0

    build(0, hank)
    lax.fori_loop(0, NBLK // CH // 2, chunks, 0)
    multiply(NBLK // CH - 1, hank)

    lane24 = lax.broadcasted_iota(jnp.int32, (ROWS, 128), 1)

    def shifted(t):
        lag = lag_ref[0, t]
        here = pres_ref[0, t].astype(F32)
        a, r = lag // 128, lag % 128
        left = right = None
        for q in range(NQ):
            at = (q * NT + t) * NBLK + q + a
            one, two = part[pl.ds(at, ROWS), :], part[pl.ds(at + 1, ROWS), :]
            left = one if left is None else left + one
            right = two if right is None else right + two
        by = (128 - r) % 128
        left, right = pltpu.roll(left, by, 1), pltpu.roll(right, by, 1)
        return jnp.where(lane24 < 128 - r, left, right) * (scl[pl.ds(t, 1), :] * here)

    def place(k):
        return (z + 4 + k // 2 - (k % 2) * k + 8) % 8

    def copy_c(k):
        return pltpu.make_async_remote_copy(
            src_ref=sendc.at[k], dst_ref=recvc.at[k], send_sem=sem_cs.at[k], recv_sem=sem_cr.at[k],
            device_id=dev(x, z, 1 - c), device_id_type=MESH)

    def copy_x(k, d):
        return pltpu.make_async_remote_copy(
            src_ref=sendx.at[k, d - 1], dst_ref=recvx.at[k, d - 1],
            send_sem=sem_xs.at[k, d - 1], recv_sem=sem_xr.at[k, d - 1],
            device_id=dev((x + d) % 4, z, c), device_id_type=MESH)

    def copy_z(k):
        return pltpu.make_async_remote_copy(
            src_ref=sendz.at[k], dst_ref=recvz.at[k], send_sem=sem_zs.at[k], recv_sem=sem_zr.at[k],
            device_id=dev(x, (z + AWAY[k]) % 8, c), device_id_type=MESH)

    def both(k, _):
        for d in range(4):
            sendc[k, d] = shifted(((x + d) % 4) * 16 + place(k) * 2 + 1 - c)
        copy_c(k).start()
        for d in range(4):
            own[k, d] = shifted(((x + d) % 4) * 16 + place(k) * 2 + c)
        return 0

    def fold(k, _):
        copy_c(k).wait_recv()
        for d in (2, 1, 3):
            sendx[k, d - 1] = own[k, d] + recvc[k, d]
            copy_x(k, d).start()
        return 0

    def both_fold(k, _):
        both(k, 0)
        fold(k - 5, 0)
        return 0

    pl.semaphore_wait(barrier, 1 + 3 + 7 + 7)
    lax.fori_loop(0, 5, both, 0)
    lax.fori_loop(5, 8, both_fold, 0)
    lax.fori_loop(3, 8, fold, 0)
    row = None
    for k in range(8):
        for d in (1, 3, 2):
            copy_x(k, d).wait_recv()
        row = (own[k, 0] + recvc[k, 0]) + (recvx[k, 0] + recvx[k, 1] + recvx[k, 2])
        if k < 7:
            sendz[k] = row
            copy_z(k).start()
    for k in range(7):
        copy_z(k).wait_recv()
        row = row + recvz[k]

    pos = jnp.clip(jnp.abs(row) * (BINS / 512.0) - 0.5, 0.0, BINS - 1.0)
    low = jnp.minimum(jnp.floor(pos), BINS - 2.0)
    high = jnp.floor(low * (1.0 / 32.0))
    inside = pos - 32.0 * high
    iota_h = lax.broadcasted_iota(jnp.int32, (32, 128), 0).astype(F32)
    iota_l = lax.broadcasted_iota(jnp.int32, (40, 128), 0).astype(F32)
    ones, hats = [], [[], [], []]
    for i in range(ROWS):
        ones.append(jnp.where(iota_h == high[i : i + 1, :], 1.0, 0.0).astype(BF16))
        hat = jnp.maximum(1.0 - jnp.abs(inside[i : i + 1, :] - iota_l), 0.0)
        for k in range(3):
            near = hat.astype(BF16)
            hats[k].append(near)
            hat = hat - near.astype(F32)
    ones = jnp.concatenate(ones, axis=1)
    counts = None
    for k in range(3):
        got_k = lax.dot_general(
            jnp.concatenate(hats[k], axis=1), ones, (((1,), (1,)), ((), ())),
            preferred_element_type=F32)
        counts = got_k if counts is None else counts + got_k
    over = jnp.concatenate([jnp.zeros((1, 1), F32), counts[32:33, 0:31]], axis=1)
    row_l = lax.broadcasted_iota(jnp.int32, (32, 32), 0)
    col_h = lax.broadcasted_iota(jnp.int32, (32, 32), 1)
    counts = counts[0:32, :] + jnp.where(row_l == 0, jnp.broadcast_to(over, (32, 32)), 0.0)
    below = jnp.where(col_h < row_l, 1.0, 0.0)
    above = jnp.where(row_l < col_h, 1.0, 0.0)
    sums = jnp.broadcast_to(jnp.sum(counts, axis=0, keepdims=True), (8, 32))
    before = jnp.dot(below, counts, precision=lax.Precision.HIGHEST, preferred_element_type=F32)
    before = before + jnp.dot(
        sums, above, precision=lax.Precision.HIGHEST, preferred_element_type=F32)[0:1, :]
    share = jnp.clip((0.5 * TOUT - before) / jnp.maximum(counts, 1.0), 0.0, 1.0)
    share = jnp.sum(jnp.sum(share, axis=1, keepdims=True), axis=0, keepdims=True)
    mad = 1.4826 * ((512.0 / BINS) * share)
    pk[...] = row / mad
    madrow = jnp.broadcast_to(mad, (8, 128))

    lane8 = lax.broadcasted_iota(jnp.int32, (8, 128), 1)
    for j in range(8):
        at, off = (OWN * j) // 128, (OWN * j) % 128
        piece = pk[pl.ds(at, 8, stride=3), :]
        if off:
            piece = pltpu.roll(piece, 128 - off, 1)
            if off + OWN > 128:
                nxt = pltpu.roll(pk[pl.ds(at + 1, 8, stride=3), :], 128 - off, 1)
                piece = jnp.where(lane8 < 128 - off, piece, nxt)
        piece = jnp.where(lane8 < OWN, piece, madrow)
        for g in range(8):
            outr[8 * g + j] = piece[g : g + 1, :]

    def copy_o(xx, zz, cc):
        to = xx * 16 + zz * 2 + cc
        return pltpu.make_async_remote_copy(
            src_ref=outr.at[to], dst_ref=got.at[s], send_sem=sem_os, recv_sem=sem_or,
            device_id=(to, tp), device_id_type=MESH)

    others = [(x + d) % 4 for d in range(4)]

    def send(k, _):
        zz = place(k)
        for d in (2, 1, 3, 0):
            copy_o(others[d], zz, c).start()
            copy_o(others[d], zz, 1 - c).start()
        return 0

    lax.fori_loop(0, 7, send, 0)
    for d in (2, 1, 3):
        copy_o(others[d], z, c).start()
        copy_o(others[d], z, 1 - c).start()
    copy_o(x, z, 1 - c).start()
    got[s] = outr[s]
    pltpu.make_async_copy(outr.at[pl.ds(0, 63)], got.at[pl.ds(0, 63)], sem_or).wait()

    best = jnp.max(got[...], axis=0)
    pkgot[0] = best

    def copy_p(d):
        return pltpu.make_async_remote_copy(
            src_ref=pkgot.at[0], dst_ref=pkgot.at[d], send_sem=sem_ps.at[d - 1],
            recv_sem=sem_pr.at[d - 1], device_id=(s, (tp + d) % 8), device_id_type=MESH)

    for d in (4, 3, 5, 2, 6, 1, 7):
        copy_p(d).start()
    flat = jnp.concatenate([got[i] for i in range(64)] + [jnp.zeros((64, 128), F32)], axis=0)
    turned = flat.T
    score_ref[...] = turned[0:OWN, 0:NT]
    mad_ref[...] = turned[OWN : OWN + 1, 0:NT]
    for d in (1, 7, 2, 6, 3, 5, 4):
        copy_p(d).wait_recv()
        best = jnp.maximum(best, pkgot[d])
    peak_ref[...] = best[:, 0:OWN]

    for k in range(8):
        copy_c(k).wait_send()
        for d in range(1, 4):
            copy_x(k, d).wait_send()
    for k in range(7):
        copy_z(k).wait_send()
        copy_p(k + 1).wait_send()
    pltpu.make_async_copy(outr.at[pl.ds(0, 63)], got.at[pl.ds(0, 63)], sem_os).wait()


def put_out(a, b, c, a_out, b_out, c_out, sems):
    copies = [
        pltpu.make_async_copy(one, two, sems.at[i])
        for i, (one, two) in enumerate(((a, a_out), (b, b_out), (c, c_out)))
    ]
    for copy in copies:
        copy.start()
    for copy in copies:
        copy.wait()


def on_device(waveform, templates, lags, present):
    vmem = pl.BlockSpec(memory_space=pltpu.VMEM)
    dma = pltpu.SemaphoreType.DMA
    hbm = pl.BlockSpec(memory_space=pltpu.HBM)
    results = pl.pallas_call(
        kernel,
        out_shape=(
            jax.ShapeDtypeStruct((OWN, NT), F32),
            jax.ShapeDtypeStruct((1, NT), F32),
            jax.ShapeDtypeStruct((1, OWN), F32),
        ),
        in_specs=[hbm, hbm, hbm, hbm],
        out_specs=(vmem, vmem, vmem),
        scratch_shapes=[
            pltpu.VMEM((CHANS, SAMPLES), BF16),
            pltpu.VMEM((NT, CHANS * LEN), BF16),
            pltpu.SMEM((1, NT), jnp.int32),
            pltpu.SMEM((1, NT), jnp.int32),
            dma((4,)),
            pltpu.VMEM((8, (NBLK + 1) * 128), F32),
            pltpu.VMEM((NQ * NT, CHANS * TAPS), BF16),
            pltpu.VMEM((CHANS * TAPS, CH * 128), BF16),
            pltpu.VMEM((CHANS * TAPS, CH * 128), BF16),
            pltpu.VMEM((NQ * NT * NBLK, 128), F32),
            pltpu.VMEM((NT, 128), F32),
            pltpu.VMEM((8, 4, ROWS, 128), F32),
            pltpu.VMEM((8, 4, ROWS, 128), F32),
            pltpu.VMEM((8, 4, ROWS, 128), F32),
            pltpu.VMEM((8, 3, ROWS, 128), F32),
            pltpu.VMEM((8, 3, ROWS, 128), F32),
            pltpu.VMEM((7, ROWS, 128), F32),
            pltpu.VMEM((7, ROWS, 128), F32),
            pltpu.VMEM((64, 1, 128), F32),
            pltpu.VMEM((64, 1, 128), F32),
            pltpu.VMEM((ROWS, 128), F32),
            pltpu.VMEM((8, 1, 128), F32),
            dma((8,)), dma((8,)), dma((8, 3)), dma((8, 3)), dma((7,)), dma((7,)),
            dma(()), dma(()), dma((7,)), dma((7,)),
        ],
        compiler_params=pltpu.CompilerParams(
            collective_id=0, has_side_effects=True, vmem_limit_bytes=56500000),
    )(waveform[0], templates[:, 0, :], lags.reshape(1, NT), present.reshape(1, NT))
    score, mad, peak = pl.pallas_call(
        put_out,
        out_shape=(
            jax.ShapeDtypeStruct((OWN, NT), F32),
            jax.ShapeDtypeStruct((1, NT), F32),
            jax.ShapeDtypeStruct((1, OWN), F32),
        ),
        in_specs=[vmem, vmem, vmem],
        out_specs=(hbm, hbm, hbm),
        scratch_shapes=[dma((3,))],
        compiler_params=pltpu.CompilerParams(vmem_limit_bytes=1024 * 1024),
    )(*results)
    return score, mad[0], peak[0]


def solution(mesh):
    return jax.shard_map(
        on_device,
        mesh=mesh,
        in_specs=(P("sta", None, None), P("tpl", "sta", None), P("tpl", "sta"), P("tpl", "sta")),
        out_specs=(P("sta", "tpl"), P("tpl"), P("sta")),
        check_vma=False,
    )
```

```python
import functools

import jax
import jax.numpy as jnp
from jax import lax
from jax.experimental import pallas as pl
from jax.experimental.pallas import tpu as pltpu
from jax.sharding import PartitionSpec as P

LEN = 512
CHANS = 3
SAMPLES = 6583
BINS = 1024
TOUT = 3072
NT = 64
TAPS = 128
NQ = 2
NBLK = 50
CH = 4
ROWS = TOUT // 128
OWN = TOUT // 64
F32 = jnp.float32
BF16 = jnp.bfloat16
MESH = pl.DeviceIdType.MESH
AWAY = (4, 3, 5, 2, 6, 1, 7, 0)


def kernel(
    wave_hbm, temp_hbm, lag_hbm, pres_hbm, score_ref, mad_ref, peak_ref,
    wave_ref, temp_ref, lag_ref, pres_ref, sem_in, wrow, amat, hank0, hank1, hank2, part, scl, sendc, own, recvc, sendx, recvx, sendz, recvz,
    outr, got, pk, pkgot,
    sem_cs, sem_cr, sem_xs, sem_xr, sem_zs, sem_zr, sem_os, sem_or, sem_ps, sem_pr,
):
    s = lax.axis_index("sta")
    tp = lax.axis_index("tpl")
    x, z, c = s // 16, (s // 2) % 8, s % 2

    def dev(xx, zz, cc):
        return (xx * 16 + zz * 2 + cc, tp)

    inputs = [
        pltpu.make_async_copy(a, b, sem_in.at[i])
        for i, (a, b) in enumerate(
            ((temp_hbm, temp_ref), (wave_hbm, wave_ref), (lag_hbm, lag_ref), (pres_hbm, pres_ref))
        )
    ]
    for copy in inputs:
        copy.start()

    barrier = pltpu.get_barrier_semaphore()
    for i in range(1, 8):
        pl.semaphore_signal(barrier, inc=1, device_id=(s, (tp + i) % 8), device_id_type=MESH)
        pl.semaphore_signal(barrier, inc=1, device_id=dev(x, (z + i) % 8, c), device_id_type=MESH)
    for i in range(1, 4):
        pl.semaphore_signal(barrier, inc=1, device_id=dev((x + i) % 4, z, c), device_id_type=MESH)
    pl.semaphore_signal(barrier, inc=1, device_id=dev(x, z, 1 - c), device_id_type=MESH)

    wrow[...] = jnp.zeros(wrow.shape, F32)
    for copy in inputs:
        copy.wait()
    wrow[0:CHANS, 0:SAMPLES] = wave_ref[...].astype(F32)

    total = jnp.zeros((NT, 128), F32)
    flip_i = lax.broadcasted_iota(jnp.int32, (128, 128), 0)
    flip_j = lax.broadcasted_iota(jnp.int32, (128, 128), 1)
    flip = jnp.where(flip_i + flip_j == 127, 1.0, 0.0).astype(BF16)
    for ch in range(CHANS):
        for k in range(LEN // TAPS):
            piece = temp_ref[:, ch * LEN + k * TAPS : ch * LEN + (k + 1) * TAPS]
            wide = piece.astype(F32)
            total = total + wide * wide
            turned = jnp.dot(piece, flip, preferred_element_type=F32).astype(BF16)
            at = (ch * 2 + k % 2) * TAPS
            amat[(k // 2) * NT : (k // 2 + 1) * NT, at : at + TAPS] = turned
    norm = jnp.sqrt(jnp.sum(total, axis=1, keepdims=True) + 1e-6)
    scl[...] = jnp.broadcast_to(1.0 / norm, (NT, 128))

    rho = lax.broadcasted_iota(jnp.int32, (16, 128), 0)
    lane16 = lax.broadcasted_iota(jnp.int32, (16, 128), 1)

    def build(j, into, ahead=None):
        for ch in range(CHANS):
            for g in range(TAPS // 16):
                rows = slice(ch * TAPS + g * 16, ch * TAPS + (g + 1) * 16)
                first = lane16 <= rho + 16 * g
                before = None
                for b in range(CH + 1):
                    at = pl.multiple_of((j * CH + b) * 128, 128)
                    row = jnp.broadcast_to(wrow[ch : ch + 1, pl.ds(at, 128)], (16, 128))
                    after = pltpu.roll(row, 1 + 16 * g, 1, stride=1, stride_axis=0)
                    if b:
                        block = jnp.where(first, before, after).astype(BF16)
                        into[rows, (b - 1) * 128 : b * 128] = block
                        if b == 1 and ahead is not None:
                            ahead[rows, CH * 128 : (CH + 1) * 128] = block
                    before = after

    def multiply(j, held, tiles=CH // 2):
        for p in range(tiles):
            halves = []
            for ch in range(CHANS):
                for h in range(2):
                    at = (2 * p + h) * 128
                    halves.append(held[ch * TAPS : (ch + 1) * TAPS, at : at + 256])
            out = jnp.dot(
                amat[...], jnp.concatenate(halves, axis=0), preferred_element_type=F32)
            for g in range(NQ * NT // 8):
                for b in range(2):
                    part[pl.ds(g * 8 * NBLK + j * CH + 2 * p + b, 8, stride=NBLK), :] = out[
                        g * 8 : (g + 1) * 8, b * 128 : (b + 1) * 128
                    ]

    def chunks(i, _):
        multiply(3 * i, hank0)
        build(3 * i + 2, hank2, hank1)
        multiply(3 * i + 1, hank1)
        build(3 * i + 3, hank0, hank2)
        multiply(3 * i + 2, hank2)
        build(3 * i + 4, hank1, hank0)
        return 0

    build(0, hank0)
    build(1, hank1, hank0)
    lax.fori_loop(0, 3, chunks, 0)
    multiply(9, hank0)
    build(11, hank2, hank1)
    multiply(10, hank1)
    build(12, hank0, hank2)
    multiply(11, hank2)
    multiply(12, hank0, 1)

    lane24 = lax.broadcasted_iota(jnp.int32, (ROWS, 128), 1)

    def shifted(t):
        lag = lag_ref[0, t]
        here = pres_ref[0, t].astype(F32)
        a, r = lag // 128, lag % 128
        left = right = None
        for q in range(NQ):
            at = (q * NT + t) * NBLK + 2 * q + a
            one, two = part[pl.ds(at, ROWS), :], part[pl.ds(at + 1, ROWS), :]
            left = one if left is None else left + one
            right = two if right is None else right + two
        by = (128 - r) % 128
        left, right = pltpu.roll(left, by, 1), pltpu.roll(right, by, 1)
        return jnp.where(lane24 < 128 - r, left, right) * (scl[pl.ds(t, 1), :] * here)

    def place(k):
        return (z + 4 + k // 2 - (k % 2) * k + 8) % 8

    def copy_c(k):
        return pltpu.make_async_remote_copy(
            src_ref=sendc.at[k], dst_ref=recvc.at[k], send_sem=sem_cs.at[k], recv_sem=sem_cr.at[k],
            device_id=dev(x, z, 1 - c), device_id_type=MESH)

    def copy_x(k, d):
        return pltpu.make_async_remote_copy(
            src_ref=sendx.at[k, d - 1], dst_ref=recvx.at[k, d - 1],
            send_sem=sem_xs.at[k, d - 1], recv_sem=sem_xr.at[k, d - 1],
            device_id=dev((x + d) % 4, z, c), device_id_type=MESH)

    def copy_z(k):
        return pltpu.make_async_remote_copy(
            src_ref=sendz.at[k], dst_ref=recvz.at[k], send_sem=sem_zs.at[k], recv_sem=sem_zr.at[k],
            device_id=dev(x, (z + AWAY[k]) % 8, c), device_id_type=MESH)

    def both(k, _):
        for d in range(4):
            sendc[k, d] = shifted(((x + d) % 4) * 16 + place(k) * 2 + 1 - c)
        copy_c(k).start()
        for d in range(4):
            own[k, d] = shifted(((x + d) % 4) * 16 + place(k) * 2 + c)
        return 0

    def fold(k, _):
        copy_c(k).wait_recv()
        for d in (2, 1, 3):
            sendx[k, d - 1] = own[k, d] + recvc[k, d]
            copy_x(k, d).start()
        return 0

    def both_fold(k, _):
        both(k, 0)
        fold(k - 5, 0)
        return 0

    pl.semaphore_wait(barrier, 1 + 3 + 7 + 7)
    lax.fori_loop(0, 5, both, 0)
    lax.fori_loop(5, 8, both_fold, 0)
    lax.fori_loop(3, 8, fold, 0)
    row = None
    for k in range(8):
        for d in (1, 3, 2):
            copy_x(k, d).wait_recv()
        row = (own[k, 0] + recvc[k, 0]) + (recvx[k, 0] + recvx[k, 1] + recvx[k, 2])
        if k < 7:
            sendz[k] = row
            copy_z(k).start()
    for k in range(7):
        copy_z(k).wait_recv()
        row = row + recvz[k]

    pos = jnp.clip(jnp.abs(row) * (BINS / 512.0) - 0.5, 0.0, BINS - 1.0)
    low = jnp.minimum(jnp.floor(pos), BINS - 2.0)
    high = jnp.floor(low * (1.0 / 32.0))
    inside = pos - 32.0 * high
    iota_h = lax.broadcasted_iota(jnp.int32, (32, 128), 0).astype(F32)
    iota_l = lax.broadcasted_iota(jnp.int32, (40, 128), 0).astype(F32)
    ones, hats = [], [[], [], []]
    for i in range(ROWS):
        ones.append(jnp.where(iota_h == high[i : i + 1, :], 1.0, 0.0).astype(BF16))
        hat = jnp.maximum(1.0 - jnp.abs(inside[i : i + 1, :] - iota_l), 0.0)
        for k in range(3):
            near = hat.astype(BF16)
            hats[k].append(near)
            hat = hat - near.astype(F32)
    ones = jnp.concatenate(ones, axis=1)
    stacked = jnp.concatenate([jnp.concatenate(piece, axis=1) for piece in hats], axis=0)
    counts = lax.dot_general(stacked, ones, (((1,), (1,)), ((), ())), preferred_element_type=F32)
    counts = counts[0:40, :] + counts[40:80, :] + counts[80:120, :]
    over = jnp.concatenate([jnp.zeros((1, 1), F32), counts[32:33, 0:31]], axis=1)
    row_l = lax.broadcasted_iota(jnp.int32, (32, 32), 0)
    col_h = lax.broadcasted_iota(jnp.int32, (32, 32), 1)
    counts = counts[0:32, :] + jnp.where(row_l == 0, jnp.broadcast_to(over, (32, 32)), 0.0)
    below = jnp.where(col_h < row_l, 1.0, 0.0)
    above = jnp.where(row_l < col_h, 1.0, 0.0)
    sums = jnp.broadcast_to(jnp.sum(counts, axis=0, keepdims=True), (8, 32))
    before = jnp.dot(below, counts, precision=lax.Precision.HIGHEST, preferred_element_type=F32)
    before = before + jnp.dot(
        sums, above, precision=lax.Precision.HIGHEST, preferred_element_type=F32)[0:1, :]
    share = jnp.clip((0.5 * TOUT - before) / jnp.maximum(counts, 1.0), 0.0, 1.0)
    share = jnp.sum(jnp.sum(share, axis=1, keepdims=True), axis=0, keepdims=True)
    mad = 1.4826 * ((512.0 / BINS) * share)
    pk[...] = row / mad
    madrow = jnp.broadcast_to(mad, (8, 128))

    lane8 = lax.broadcasted_iota(jnp.int32, (8, 128), 1)
    for j in range(8):
        at, off = (OWN * j) // 128, (OWN * j) % 128
        piece = pk[pl.ds(at, 8, stride=3), :]
        if off:
            piece = pltpu.roll(piece, 128 - off, 1)
            if off + OWN > 128:
                nxt = pltpu.roll(pk[pl.ds(at + 1, 8, stride=3), :], 128 - off, 1)
                piece = jnp.where(lane8 < 128 - off, piece, nxt)
        piece = jnp.where(lane8 < OWN, piece, madrow)
        for g in range(8):
            outr[8 * g + j] = piece[g : g + 1, :]

    def copy_o(xx, zz, cc):
        to = xx * 16 + zz * 2 + cc
        return pltpu.make_async_remote_copy(
            src_ref=outr.at[to], dst_ref=got.at[s], send_sem=sem_os, recv_sem=sem_or,
            device_id=(to, tp), device_id_type=MESH)

    others = [(x + d) % 4 for d in range(4)]

    def send(k, _):
        zz = place(k)
        for d in (2, 1, 3, 0):
            copy_o(others[d], zz, c).start()
            copy_o(others[d], zz, 1 - c).start()
        return 0

    lax.fori_loop(0, 7, send, 0)
    for d in (2, 1, 3):
        copy_o(others[d], z, c).start()
        copy_o(others[d], z, 1 - c).start()
    copy_o(x, z, 1 - c).start()
    got[s] = outr[s]
    pltpu.make_async_copy(outr.at[pl.ds(0, 63)], got.at[pl.ds(0, 63)], sem_or).wait()

    best = jnp.max(got[...], axis=0)
    pkgot[0] = best

    def copy_p(d):
        return pltpu.make_async_remote_copy(
            src_ref=pkgot.at[0], dst_ref=pkgot.at[d], send_sem=sem_ps.at[d - 1],
            recv_sem=sem_pr.at[d - 1], device_id=(s, (tp + d) % 8), device_id_type=MESH)

    for d in (4, 3, 5, 2, 6, 1, 7):
        copy_p(d).start()
    flat = jnp.concatenate([got[i] for i in range(64)] + [jnp.zeros((64, 128), F32)], axis=0)
    turned = flat.T
    score_ref[...] = turned[0:OWN, 0:NT]
    mad_ref[...] = turned[OWN : OWN + 1, 0:NT]
    for d in (1, 7, 2, 6, 3, 5, 4):
        copy_p(d).wait_recv()
        best = jnp.maximum(best, pkgot[d])
    peak_ref[...] = best[:, 0:OWN]

    for k in range(8):
        copy_c(k).wait_send()
        for d in range(1, 4):
            copy_x(k, d).wait_send()
    for k in range(7):
        copy_z(k).wait_send()
        copy_p(k + 1).wait_send()
    pltpu.make_async_copy(outr.at[pl.ds(0, 63)], got.at[pl.ds(0, 63)], sem_os).wait()


def put_out(a, b, c, a_out, b_out, c_out, sems):
    copies = [
        pltpu.make_async_copy(one, two, sems.at[i])
        for i, (one, two) in enumerate(((a, a_out), (b, b_out), (c, c_out)))
    ]
    for copy in copies:
        copy.start()
    for copy in copies:
        copy.wait()


def on_device(waveform, templates, lags, present):
    vmem = pl.BlockSpec(memory_space=pltpu.VMEM)
    dma = pltpu.SemaphoreType.DMA
    hbm = pl.BlockSpec(memory_space=pltpu.HBM)
    results = pl.pallas_call(
        kernel,
        out_shape=(
            jax.ShapeDtypeStruct((OWN, NT), F32),
            jax.ShapeDtypeStruct((1, NT), F32),
            jax.ShapeDtypeStruct((1, OWN), F32),
        ),
        in_specs=[hbm, hbm, hbm, hbm],
        out_specs=(vmem, vmem, vmem),
        scratch_shapes=[
            pltpu.VMEM((CHANS, SAMPLES), BF16),
            pltpu.VMEM((NT, CHANS * LEN), BF16),
            pltpu.SMEM((1, NT), jnp.int32),
            pltpu.SMEM((1, NT), jnp.int32),
            dma((4,)),
            pltpu.VMEM((8, 53 * 128), F32),
            pltpu.VMEM((NQ * NT, 2 * CHANS * TAPS), BF16),
            pltpu.VMEM((CHANS * TAPS, (CH + 1) * 128), BF16),
            pltpu.VMEM((CHANS * TAPS, (CH + 1) * 128), BF16),
            pltpu.VMEM((CHANS * TAPS, (CH + 1) * 128), BF16),
            pltpu.VMEM((NQ * NT * NBLK, 128), F32),
            pltpu.VMEM((NT, 128), F32),
            pltpu.VMEM((8, 4, ROWS, 128), F32),
            pltpu.VMEM((8, 4, ROWS, 128), F32),
            pltpu.VMEM((8, 4, ROWS, 128), F32),
            pltpu.VMEM((8, 3, ROWS, 128), F32),
            pltpu.VMEM((8, 3, ROWS, 128), F32),
            pltpu.VMEM((7, ROWS, 128), F32),
            pltpu.VMEM((7, ROWS, 128), F32),
            pltpu.VMEM((64, 1, 128), F32),
            pltpu.VMEM((64, 1, 128), F32),
            pltpu.VMEM((ROWS, 128), F32),
            pltpu.VMEM((8, 1, 128), F32),
            dma((8,)), dma((8,)), dma((8, 3)), dma((8, 3)), dma((7,)), dma((7,)),
            dma(()), dma(()), dma((7,)), dma((7,)),
        ],
        compiler_params=pltpu.CompilerParams(
            collective_id=0, has_side_effects=True, vmem_limit_bytes=56500000),
    )(waveform[0], templates[:, 0, :], lags.reshape(1, NT), present.reshape(1, NT))
    score, mad, peak = pl.pallas_call(
        put_out,
        out_shape=(
            jax.ShapeDtypeStruct((OWN, NT), F32),
            jax.ShapeDtypeStruct((1, NT), F32),
            jax.ShapeDtypeStruct((1, OWN), F32),
        ),
        in_specs=[vmem, vmem, vmem],
        out_specs=(hbm, hbm, hbm),
        scratch_shapes=[dma((3,))],
        compiler_params=pltpu.CompilerParams(vmem_limit_bytes=1024 * 1024),
    )(*results)
    return score, mad[0], peak[0]


def solution(mesh):
    return jax.shard_map(
        on_device,
        mesh=mesh,
        in_specs=(P("sta", None, None), P("tpl", "sta", None), P("tpl", "sta"), P("tpl", "sta")),
        out_specs=(P("sta", "tpl"), P("tpl"), P("sta")),
        check_vma=False,
    )
```

```python
import functools

import jax
import jax.numpy as jnp
from jax import lax
from jax.experimental import pallas as pl
from jax.experimental.pallas import tpu as pltpu
from jax.sharding import PartitionSpec as P

LEN = 512
CHANS = 3
SAMPLES = 6583
BINS = 1024
TOUT = 3072
NT = 64
TAPS = 128
NQ = 2
NBLK = 50
CH = 4
ROWS = TOUT // 128
OWN = TOUT // 64
F32 = jnp.float32
BF16 = jnp.bfloat16
MESH = pl.DeviceIdType.MESH
AWAY = (4, 3, 5, 2, 6, 1, 7, 0)
VIA = (None, None, 3, 3, 1, 3, 1, 3)


def kernel(
    wave_hbm, temp_hbm, lag_hbm, pres_hbm, score_ref, mad_ref, peak_ref,
    wave_ref, temp_ref, lag_ref, pres_ref, sem_in, wrow, amat, hank0, hank1, hank2, part, scl, sendc, own, recvc, sendx, recvx, recvr, sendz, recvz,
    outr, got, pk, pkgot,
    sem_cs, sem_cr, sem_xs, sem_xr, sem_rs, sem_rr, sem_zs, sem_zr, sem_os, sem_or, sem_ps, sem_pr,
):
    s = lax.axis_index("sta")
    tp = lax.axis_index("tpl")
    x, z, c = s // 16, (s // 2) % 8, s % 2

    def dev(xx, zz, cc):
        return (xx * 16 + zz * 2 + cc, tp)

    inputs = [
        pltpu.make_async_copy(a, b, sem_in.at[i])
        for i, (a, b) in enumerate(
            ((temp_hbm, temp_ref), (wave_hbm, wave_ref), (lag_hbm, lag_ref), (pres_hbm, pres_ref))
        )
    ]
    for copy in inputs:
        copy.start()

    barrier = pltpu.get_barrier_semaphore()
    for i in range(1, 8):
        pl.semaphore_signal(barrier, inc=1, device_id=(s, (tp + i) % 8), device_id_type=MESH)
        pl.semaphore_signal(barrier, inc=1, device_id=dev(x, (z + i) % 8, c), device_id_type=MESH)
    for i in range(1, 4):
        pl.semaphore_signal(barrier, inc=1, device_id=dev((x + i) % 4, z, c), device_id_type=MESH)
    pl.semaphore_signal(barrier, inc=1, device_id=dev(x, z, 1 - c), device_id_type=MESH)

    wrow[...] = jnp.zeros(wrow.shape, F32)
    for copy in inputs:
        copy.wait()
    wrow[0:CHANS, 0:SAMPLES] = wave_ref[...].astype(F32)

    total = jnp.zeros((NT, 128), F32)
    flip_i = lax.broadcasted_iota(jnp.int32, (128, 128), 0)
    flip_j = lax.broadcasted_iota(jnp.int32, (128, 128), 1)
    flip = jnp.where(flip_i + flip_j == 127, 1.0, 0.0).astype(BF16)
    for ch in range(CHANS):
        for k in range(LEN // TAPS):
            piece = temp_ref[:, ch * LEN + k * TAPS : ch * LEN + (k + 1) * TAPS]
            wide = piece.astype(F32)
            total = total + wide * wide
            turned = jnp.dot(piece, flip, preferred_element_type=F32).astype(BF16)
            at = (ch * 2 + k % 2) * TAPS
            amat[(k // 2) * NT : (k // 2 + 1) * NT, at : at + TAPS] = turned
    norm = jnp.sqrt(jnp.sum(total, axis=1, keepdims=True) + 1e-6)
    scl[...] = jnp.broadcast_to(1.0 / norm, (NT, 128))

    rho = lax.broadcasted_iota(jnp.int32, (16, 128), 0)
    lane16 = lax.broadcasted_iota(jnp.int32, (16, 128), 1)

    def build(j, into, ahead=None):
        for ch in range(CHANS):
            for g in range(TAPS // 16):
                rows = slice(ch * TAPS + g * 16, ch * TAPS + (g + 1) * 16)
                first = lane16 <= rho + 16 * g
                before = None
                for b in range(CH + 1):
                    at = pl.multiple_of((j * CH + b) * 128, 128)
                    row = jnp.broadcast_to(wrow[ch : ch + 1, pl.ds(at, 128)], (16, 128))
                    after = pltpu.roll(row, 1 + 16 * g, 1, stride=1, stride_axis=0)
                    if b:
                        block = jnp.where(first, before, after).astype(BF16)
                        into[rows, (b - 1) * 128 : b * 128] = block
                        if b == 1 and ahead is not None:
                            ahead[rows, CH * 128 : (CH + 1) * 128] = block
                    before = after

    def multiply(j, held, tiles=CH // 2):
        for p in range(tiles):
            halves = []
            for ch in range(CHANS):
                for h in range(2):
                    at = (2 * p + h) * 128
                    halves.append(held[ch * TAPS : (ch + 1) * TAPS, at : at + 256])
            out = jnp.dot(
                amat[...], jnp.concatenate(halves, axis=0), preferred_element_type=F32)
            for g in range(NQ * NT // 8):
                for b in range(2):
                    part[pl.ds(g * 8 * NBLK + j * CH + 2 * p + b, 8, stride=NBLK), :] = out[
                        g * 8 : (g + 1) * 8, b * 128 : (b + 1) * 128
                    ]

    def chunks(i, _):
        multiply(3 * i, hank0)
        build(3 * i + 2, hank2, hank1)
        multiply(3 * i + 1, hank1)
        build(3 * i + 3, hank0, hank2)
        multiply(3 * i + 2, hank2)
        build(3 * i + 4, hank1, hank0)
        return 0

    build(0, hank0)
    build(1, hank1, hank0)
    lax.fori_loop(0, 3, chunks, 0)
    multiply(9, hank0)
    build(11, hank2, hank1)
    multiply(10, hank1)
    build(12, hank0, hank2)
    multiply(11, hank2)
    multiply(12, hank0, 1)

    lane24 = lax.broadcasted_iota(jnp.int32, (ROWS, 128), 1)

    def shifted(t):
        lag = lag_ref[0, t]
        here = pres_ref[0, t].astype(F32)
        a, r = lax.shift_right_logical(lag, 7), lax.bitwise_and(lag, 127)
        left = right = None
        for q in range(NQ):
            at = (q * NT + t) * NBLK + 2 * q + a
            one, two = part[pl.ds(at, ROWS), :], part[pl.ds(at + 1, ROWS), :]
            left = one if left is None else left + one
            right = two if right is None else right + two
        by = lax.bitwise_and(128 - r, 127)
        left, right = pltpu.roll(left, by, 1), pltpu.roll(right, by, 1)
        return jnp.where(lane24 < 128 - r, left, right) * (scl[pl.ds(t, 1), :] * here)

    def place(k):
        return (z + 4 + k // 2 - (k % 2) * k + 8) % 8

    beyond = [(z + AWAY[k]) % 8 for k in range(8)]
    others = [(x + d) % 4 for d in range(4)]
    group = [others[d] * 16 for d in range(4)]

    def copy_c(k):
        return pltpu.make_async_remote_copy(
            src_ref=sendc.at[k], dst_ref=recvc.at[k], send_sem=sem_cs.at[k], recv_sem=sem_cr.at[k],
            device_id=dev(x, z, 1 - c), device_id_type=MESH)

    def copy_x(k, d):
        return pltpu.make_async_remote_copy(
            src_ref=sendx.at[k, d - 1], dst_ref=recvx.at[k, d - 1],
            send_sem=sem_xs.at[k, d - 1], recv_sem=sem_xr.at[k, d - 1],
            device_id=dev(others[d], z, c), device_id_type=MESH)

    def copy_r(k):
        return pltpu.make_async_remote_copy(
            src_ref=sendx.at[k, 1], dst_ref=recvr.at[k], send_sem=sem_rs.at[k],
            recv_sem=sem_rr.at[k], device_id=dev(others[VIA[k]], z, c), device_id_type=MESH)

    def copy_z(k):
        return pltpu.make_async_remote_copy(
            src_ref=sendz.at[k], dst_ref=recvz.at[k], send_sem=sem_zs.at[k], recv_sem=sem_zr.at[k],
            device_id=dev(x, beyond[k], c), device_id_type=MESH)

    def both(k):
        at = beyond[k] * 2
        for d in range(4):
            sendc[k, d] = shifted(group[d] + at + 1 - c)
        copy_c(k).start()
        for d in range(4):
            own[k, d] = shifted(group[d] + at + c)

    def fold(k):
        copy_c(k).wait_recv()
        for d in (2, 1, 3):
            if d != VIA[k]:
                sendx[k, d - 1] = own[k, d] + recvc[k, d]
                (copy_r(k) if d == 2 and VIA[k] else copy_x(k, d)).start()

    def relay(k):
        copy_r(k).wait_recv()
        d = VIA[k]
        sendx[k, d - 1] = (own[k, d] + recvc[k, d]) + recvr[k]
        copy_x(k, d).start()

    def reduced(k):
        total = own[k, 0] + recvc[k, 0]
        for d in (1, 3) if VIA[k] else (1, 3, 2):
            copy_x(k, d).wait_recv()
            total = total + recvx[k, d - 1]
        if k < 7:
            sendz[k] = total
            copy_z(k).start()
        return total

    pl.semaphore_wait(barrier, 1 + 3 + 7 + 7)
    for k in range(8):
        both(k)
        if k >= 5:
            fold(k - 5)
    for k in range(3, 8):
        fold(k)
    relay(2)
    reduced(0)
    relay(3)
    reduced(1)
    for k in range(4, 8):
        relay(k)
    for k in range(2, 7):
        reduced(k)
    row = reduced(7)
    for k in range(7):
        copy_z(k).wait_recv()
        row = row + recvz[k]

    pos = jnp.clip(jnp.abs(row) * (BINS / 512.0) - 0.5, 0.0, BINS - 1.0)
    low = jnp.minimum(jnp.floor(pos), BINS - 2.0)
    high = jnp.floor(low * (1.0 / 32.0))
    inside = pos - 32.0 * high
    iota_h = lax.broadcasted_iota(jnp.int32, (32, 128), 0).astype(F32)
    iota_l = lax.broadcasted_iota(jnp.int32, (40, 128), 0).astype(F32)
    ones, hats = [], [[], [], []]
    for i in range(ROWS):
        ones.append(jnp.where(iota_h == high[i : i + 1, :], 1.0, 0.0).astype(BF16))
        hat = jnp.maximum(1.0 - jnp.abs(inside[i : i + 1, :] - iota_l), 0.0)
        for k in range(3):
            near = hat.astype(BF16)
            hats[k].append(near)
            hat = hat - near.astype(F32)
    ones = jnp.concatenate(ones, axis=1)
    stacked = jnp.concatenate([jnp.concatenate(piece, axis=1) for piece in hats], axis=0)
    counts = lax.dot_general(stacked, ones, (((1,), (1,)), ((), ())), preferred_element_type=F32)
    counts = counts[0:40, :] + counts[40:80, :] + counts[80:120, :]
    over = jnp.concatenate([jnp.zeros((1, 1), F32), counts[32:33, 0:31]], axis=1)
    row_l = lax.broadcasted_iota(jnp.int32, (32, 32), 0)
    col_h = lax.broadcasted_iota(jnp.int32, (32, 32), 1)
    counts = counts[0:32, :] + jnp.where(row_l == 0, jnp.broadcast_to(over, (32, 32)), 0.0)
    below = jnp.where(col_h < row_l, 1.0, 0.0)
    above = jnp.where(row_l < col_h, 1.0, 0.0)
    sums = jnp.broadcast_to(jnp.sum(counts, axis=0, keepdims=True), (8, 32))
    before = jnp.dot(below, counts, precision=lax.Precision.HIGHEST, preferred_element_type=F32)
    before = before + jnp.dot(
        sums, above, precision=lax.Precision.HIGHEST, preferred_element_type=F32)[0:1, :]
    share = jnp.clip((0.5 * TOUT - before) / jnp.maximum(counts, 1.0), 0.0, 1.0)
    share = jnp.sum(jnp.sum(share, axis=1, keepdims=True), axis=0, keepdims=True)
    mad = 1.4826 * ((512.0 / BINS) * share)
    pk[...] = row / mad
    madrow = jnp.broadcast_to(mad, (8, 128))

    lane8 = lax.broadcasted_iota(jnp.int32, (8, 128), 1)
    for j in range(8):
        at, off = (OWN * j) // 128, (OWN * j) % 128
        piece = pk[pl.ds(at, 8, stride=3), :]
        if off:
            piece = pltpu.roll(piece, 128 - off, 1)
            if off + OWN > 128:
                nxt = pltpu.roll(pk[pl.ds(at + 1, 8, stride=3), :], 128 - off, 1)
                piece = jnp.where(lane8 < 128 - off, piece, nxt)
        piece = jnp.where(lane8 < OWN, piece, madrow)
        for g in range(8):
            outr[8 * g + j] = piece[g : g + 1, :]

    def copy_o(xx, zz, cc):
        to = xx * 16 + zz * 2 + cc
        return pltpu.make_async_remote_copy(
            src_ref=outr.at[to], dst_ref=got.at[s], send_sem=sem_os, recv_sem=sem_or,
            device_id=(to, tp), device_id_type=MESH)

    def send(k, _):
        zz = place(k)
        for d in (2, 1, 3, 0):
            copy_o(others[d], zz, c).start()
            copy_o(others[d], zz, 1 - c).start()
        return 0

    lax.fori_loop(0, 7, send, 0)
    for d in (2, 1, 3):
        copy_o(others[d], z, c).start()
        copy_o(others[d], z, 1 - c).start()
    copy_o(x, z, 1 - c).start()
    got[s] = outr[s]
    pltpu.make_async_copy(outr.at[pl.ds(0, 63)], got.at[pl.ds(0, 63)], sem_or).wait()

    best = jnp.max(got[...], axis=0)
    pkgot[0] = best

    def copy_p(d):
        return pltpu.make_async_remote_copy(
            src_ref=pkgot.at[0], dst_ref=pkgot.at[d], send_sem=sem_ps.at[d - 1],
            recv_sem=sem_pr.at[d - 1], device_id=(s, (tp + d) % 8), device_id_type=MESH)

    for d in (4, 3, 5, 2, 6, 1, 7):
        copy_p(d).start()
    flat = jnp.concatenate([got[i] for i in range(64)] + [jnp.zeros((64, 128), F32)], axis=0)
    turned = flat.T
    score_ref[...] = turned[0:OWN, 0:NT]
    mad_ref[...] = turned[OWN : OWN + 1, 0:NT]
    for d in (1, 7, 2, 6, 3, 5, 4):
        copy_p(d).wait_recv()
        best = jnp.maximum(best, pkgot[d])
    peak_ref[...] = best[:, 0:OWN]

    for k in range(8):
        copy_c(k).wait_send()
        for d in range(1, 4):
            (copy_r(k) if d == 2 and VIA[k] else copy_x(k, d)).wait_send()
    for k in range(7):
        copy_z(k).wait_send()
        copy_p(k + 1).wait_send()
    pltpu.make_async_copy(outr.at[pl.ds(0, 63)], got.at[pl.ds(0, 63)], sem_os).wait()


def put_out(a, b, c, a_out, b_out, c_out, sems):
    copies = [
        pltpu.make_async_copy(one, two, sems.at[i])
        for i, (one, two) in enumerate(((a, a_out), (b, b_out), (c, c_out)))
    ]
    for copy in copies:
        copy.start()
    for copy in copies:
        copy.wait()


def on_device(waveform, templates, lags, present):
    vmem = pl.BlockSpec(memory_space=pltpu.VMEM)
    dma = pltpu.SemaphoreType.DMA
    hbm = pl.BlockSpec(memory_space=pltpu.HBM)
    results = pl.pallas_call(
        kernel,
        out_shape=(
            jax.ShapeDtypeStruct((OWN, NT), F32),
            jax.ShapeDtypeStruct((1, NT), F32),
            jax.ShapeDtypeStruct((1, OWN), F32),
        ),
        in_specs=[hbm, hbm, hbm, hbm],
        out_specs=(vmem, vmem, vmem),
        scratch_shapes=[
            pltpu.VMEM((CHANS, SAMPLES), BF16),
            pltpu.VMEM((NT, CHANS * LEN), BF16),
            pltpu.SMEM((1, NT), jnp.int32),
            pltpu.SMEM((1, NT), jnp.int32),
            dma((4,)),
            pltpu.VMEM((8, 53 * 128), F32),
            pltpu.VMEM((NQ * NT, 2 * CHANS * TAPS), BF16),
            pltpu.VMEM((CHANS * TAPS, (CH + 1) * 128), BF16),
            pltpu.VMEM((CHANS * TAPS, (CH + 1) * 128), BF16),
            pltpu.VMEM((CHANS * TAPS, (CH + 1) * 128), BF16),
            pltpu.VMEM((NQ * NT * NBLK, 128), F32),
            pltpu.VMEM((NT, 128), F32),
            pltpu.VMEM((8, 4, ROWS, 128), F32),
            pltpu.VMEM((8, 4, ROWS, 128), F32),
            pltpu.VMEM((8, 4, ROWS, 128), F32),
            pltpu.VMEM((8, 3, ROWS, 128), F32),
            pltpu.VMEM((8, 3, ROWS, 128), F32),
            pltpu.VMEM((8, ROWS, 128), F32),
            pltpu.VMEM((7, ROWS, 128), F32),
            pltpu.VMEM((7, ROWS, 128), F32),
            pltpu.VMEM((64, 1, 128), F32),
            pltpu.VMEM((64, 1, 128), F32),
            pltpu.VMEM((ROWS, 128), F32),
            pltpu.VMEM((8, 1, 128), F32),
            dma((8,)), dma((8,)), dma((8, 3)), dma((8, 3)), dma((8,)), dma((8,)),
            dma((7,)), dma((7,)),
            dma(()), dma(()), dma((7,)), dma((7,)),
        ],
        compiler_params=pltpu.CompilerParams(
            collective_id=0, has_side_effects=True, vmem_limit_bytes=56500000),
    )(waveform[0], templates[:, 0, :], lags.reshape(1, NT), present.reshape(1, NT))
    score, mad, peak = pl.pallas_call(
        put_out,
        out_shape=(
            jax.ShapeDtypeStruct((OWN, NT), F32),
            jax.ShapeDtypeStruct((1, NT), F32),
            jax.ShapeDtypeStruct((1, OWN), F32),
        ),
        in_specs=[vmem, vmem, vmem],
        out_specs=(hbm, hbm, hbm),
        scratch_shapes=[dma((3,))],
        compiler_params=pltpu.CompilerParams(vmem_limit_bytes=1024 * 1024),
    )(*results)
    return score, mad[0], peak[0]


def solution(mesh):
    return jax.shard_map(
        on_device,
        mesh=mesh,
        in_specs=(P("sta", None, None), P("tpl", "sta", None), P("tpl", "sta"), P("tpl", "sta")),
        out_specs=(P("sta", "tpl"), P("tpl"), P("sta")),
        check_vma=False,
    )
```

```python
import functools

import jax
import jax.numpy as jnp
from jax import lax
from jax.experimental import pallas as pl
from jax.experimental.pallas import tpu as pltpu
from jax.sharding import PartitionSpec as P

LEN = 512
CHANS = 3
SAMPLES = 6583
BINS = 1024
TOUT = 3072
NT = 64
TAPS = 128
NQ = 2
NBLK = 50
CH = 4
ROWS = TOUT // 128
OWN = TOUT // 64
F32 = jnp.float32
BF16 = jnp.bfloat16
MESH = pl.DeviceIdType.MESH
AWAY = (4, 3, 5, 2, 6, 1, 7, 0)


def kernel(
    wave_hbm, temp_hbm, lag_hbm, pres_hbm, score_ref, mad_ref, peak_ref,
    wave_ref, temp_ref, lag_ref, pres_ref, sem_in, wrow, amat, hank0, hank1, hank2, part, scl, sendc, own, recvc, sendx, recvx, sendz, recvz,
    outr, got, pk, pkgot,
    sem_cs, sem_cr, sem_xs, sem_xr, sem_zs, sem_zr, sem_os, sem_or, sem_ps, sem_pr,
):
    s = lax.axis_index("sta")
    tp = lax.axis_index("tpl")
    x, z, c = s // 16, (s // 2) % 8, s % 2

    def dev(xx, zz, cc):
        return (xx * 16 + zz * 2 + cc, tp)

    inputs = [
        pltpu.make_async_copy(a, b, sem_in.at[i])
        for i, (a, b) in enumerate(
            ((temp_hbm, temp_ref), (wave_hbm, wave_ref), (lag_hbm, lag_ref), (pres_hbm, pres_ref))
        )
    ]
    for copy in inputs:
        copy.start()

    barrier = pltpu.get_barrier_semaphore()
    for i in range(1, 8):
        pl.semaphore_signal(barrier, inc=1, device_id=(s, (tp + i) % 8), device_id_type=MESH)
        pl.semaphore_signal(barrier, inc=1, device_id=dev(x, (z + i) % 8, c), device_id_type=MESH)
    for i in range(1, 4):
        pl.semaphore_signal(barrier, inc=1, device_id=dev((x + i) % 4, z, c), device_id_type=MESH)
    pl.semaphore_signal(barrier, inc=1, device_id=dev(x, z, 1 - c), device_id_type=MESH)

    wrow[...] = jnp.zeros(wrow.shape, F32)
    inputs[1].wait()
    wrow[0:CHANS, 0:SAMPLES] = wave_ref[...].astype(F32)

    rho = lax.broadcasted_iota(jnp.int32, (16, 128), 0)
    lane16 = lax.broadcasted_iota(jnp.int32, (16, 128), 1)

    def build(j, into, ahead=None):
        for ch in range(CHANS):
            for g in range(TAPS // 16):
                rows = slice(ch * TAPS + g * 16, ch * TAPS + (g + 1) * 16)
                first = lane16 <= rho + 16 * g
                before = None
                for b in range(CH + 1):
                    at = pl.multiple_of((j * CH + b) * 128, 128)
                    row = jnp.broadcast_to(wrow[ch : ch + 1, pl.ds(at, 128)], (16, 128))
                    after = pltpu.roll(row, 1 + 16 * g, 1, stride=1, stride_axis=0)
                    if b:
                        block = jnp.where(first, before, after).astype(BF16)
                        into[rows, (b - 1) * 128 : b * 128] = block
                        if b == 1 and ahead is not None:
                            ahead[rows, CH * 128 : (CH + 1) * 128] = block
                    before = after

    def multiply(j, held, tiles=CH // 2):
        for p in range(tiles):
            halves = []
            for ch in range(CHANS):
                for h in range(2):
                    at = (2 * p + h) * 128
                    halves.append(held[ch * TAPS : (ch + 1) * TAPS, at : at + 256])
            out = jnp.dot(
                amat[...], jnp.concatenate(halves, axis=0), preferred_element_type=F32)
            for g in range(NQ * NT // 8):
                for b in range(2):
                    part[pl.ds(g * 8 * NBLK + j * CH + 2 * p + b, 8, stride=NBLK), :] = out[
                        g * 8 : (g + 1) * 8, b * 128 : (b + 1) * 128
                    ]

    def chunks(i, _):
        multiply(3 * i, hank0)
        build(3 * i + 2, hank2, hank1)
        multiply(3 * i + 1, hank1)
        build(3 * i + 3, hank0, hank2)
        multiply(3 * i + 2, hank2)
        build(3 * i + 4, hank1, hank0)
        return 0

    build(0, hank0)
    build(1, hank1, hank0)
    inputs[0].wait()
    inputs[2].wait()
    inputs[3].wait()

    total = jnp.zeros((NT, 128), F32)
    flip_i = lax.broadcasted_iota(jnp.int32, (128, 128), 0)
    flip_j = lax.broadcasted_iota(jnp.int32, (128, 128), 1)
    flip = jnp.where(flip_i + flip_j == 127, 1.0, 0.0).astype(BF16)
    for ch in range(CHANS):
        for k in range(LEN // TAPS):
            piece = temp_ref[:, ch * LEN + k * TAPS : ch * LEN + (k + 1) * TAPS]
            wide = piece.astype(F32)
            total = total + wide * wide
            turned = jnp.dot(piece, flip, preferred_element_type=F32).astype(BF16)
            at = (ch * 2 + k % 2) * TAPS
            amat[(k // 2) * NT : (k // 2 + 1) * NT, at : at + TAPS] = turned
    norm = jnp.sqrt(jnp.sum(total, axis=1, keepdims=True) + 1e-6)
    scl[...] = jnp.broadcast_to(1.0 / norm, (NT, 128))
    lax.fori_loop(0, 3, chunks, 0)
    multiply(9, hank0)
    build(11, hank2, hank1)
    multiply(10, hank1)
    build(12, hank0, hank2)
    multiply(11, hank2)
    multiply(12, hank0, 1)

    lane24 = lax.broadcasted_iota(jnp.int32, (ROWS, 128), 1)

    def shifted(t):
        lag = lag_ref[0, t]
        here = pres_ref[0, t].astype(F32)
        a, r = lax.shift_right_logical(lag, 7), lax.bitwise_and(lag, 127)
        left = right = None
        for q in range(NQ):
            at = (q * NT + t) * NBLK + 2 * q + a
            one, two = part[pl.ds(at, ROWS), :], part[pl.ds(at + 1, ROWS), :]
            left = one if left is None else left + one
            right = two if right is None else right + two
        by = lax.bitwise_and(128 - r, 127)
        left, right = pltpu.roll(left, by, 1), pltpu.roll(right, by, 1)
        return jnp.where(lane24 < 128 - r, left, right) * (scl[pl.ds(t, 1), :] * here)

    def place(k):
        return (z + 4 + k // 2 - (k % 2) * k + 8) % 8

    beyond = [(z + AWAY[k]) % 8 for k in range(8)]
    others = [(x + d) % 4 for d in range(4)]
    group = [others[d] * 16 for d in range(4)]

    def copy_c(k):
        return pltpu.make_async_remote_copy(
            src_ref=sendc.at[k], dst_ref=recvc.at[k], send_sem=sem_cs.at[k], recv_sem=sem_cr.at[k],
            device_id=dev(x, z, 1 - c), device_id_type=MESH)

    def copy_x(k, d):
        return pltpu.make_async_remote_copy(
            src_ref=sendx.at[k, d - 1], dst_ref=recvx.at[k, d - 1],
            send_sem=sem_xs.at[k, d - 1], recv_sem=sem_xr.at[k, d - 1],
            device_id=dev(others[d], z, c), device_id_type=MESH)

    def copy_z(k):
        return pltpu.make_async_remote_copy(
            src_ref=sendz.at[k], dst_ref=recvz.at[k], send_sem=sem_zs.at[k], recv_sem=sem_zr.at[k],
            device_id=dev(x, beyond[k], c), device_id_type=MESH)

    def both(k):
        at = beyond[k] * 2
        for d in range(4):
            sendc[k, d] = shifted(group[d] + at + 1 - c)
        copy_c(k).start()
        for d in range(4):
            own[k, d] = shifted(group[d] + at + c)

    def fold(k):
        copy_c(k).wait_recv()
        for d in (2, 1, 3):
            sendx[k, d - 1] = own[k, d] + recvc[k, d]
            copy_x(k, d).start()

    def reduced(k):
        total = own[k, 0] + recvc[k, 0]
        for d in (1, 3, 2):
            copy_x(k, d).wait_recv()
            total = total + recvx[k, d - 1]
        if k < 7:
            sendz[k] = total
            copy_z(k).start()
        return total

    pl.semaphore_wait(barrier, 1 + 3 + 7 + 7)
    for k in range(8):
        both(k)
        if k >= 5:
            fold(k - 5)
    for k in range(3, 8):
        fold(k)
    for k in range(7):
        reduced(k)
    row = reduced(7)
    for k in range(7):
        copy_z(k).wait_recv()
        row = row + recvz[k]

    pos = jnp.clip(jnp.abs(row) * (BINS / 512.0) - 0.5, 0.0, BINS - 1.0)
    low = jnp.minimum(jnp.floor(pos), BINS - 2.0)
    high = jnp.floor(low * (1.0 / 32.0))
    inside = pos - 32.0 * high
    iota_h = lax.broadcasted_iota(jnp.int32, (32, 128), 0).astype(F32)
    iota_l = lax.broadcasted_iota(jnp.int32, (40, 128), 0).astype(F32)
    ones, hats = [], [[], [], []]
    for i in range(ROWS):
        ones.append(jnp.where(iota_h == high[i : i + 1, :], 1.0, 0.0).astype(BF16))
        hat = jnp.maximum(1.0 - jnp.abs(inside[i : i + 1, :] - iota_l), 0.0)
        for k in range(3):
            near = hat.astype(BF16)
            hats[k].append(near)
            hat = hat - near.astype(F32)
    ones = jnp.concatenate(ones, axis=1)
    stacked = jnp.concatenate([jnp.concatenate(piece, axis=1) for piece in hats], axis=0)
    counts = lax.dot_general(stacked, ones, (((1,), (1,)), ((), ())), preferred_element_type=F32)
    counts = counts[0:40, :] + counts[40:80, :] + counts[80:120, :]
    over = jnp.concatenate([jnp.zeros((1, 1), F32), counts[32:33, 0:31]], axis=1)
    row_l = lax.broadcasted_iota(jnp.int32, (32, 32), 0)
    col_h = lax.broadcasted_iota(jnp.int32, (32, 32), 1)
    counts = counts[0:32, :] + jnp.where(row_l == 0, jnp.broadcast_to(over, (32, 32)), 0.0)
    below = jnp.where(col_h < row_l, 1.0, 0.0)
    above = jnp.where(row_l < col_h, 1.0, 0.0)
    sums = jnp.broadcast_to(jnp.sum(counts, axis=0, keepdims=True), (8, 32))
    before = jnp.dot(below, counts, precision=lax.Precision.HIGHEST, preferred_element_type=F32)
    before = before + jnp.dot(
        sums, above, precision=lax.Precision.HIGHEST, preferred_element_type=F32)[0:1, :]
    share = jnp.clip((0.5 * TOUT - before) / jnp.maximum(counts, 1.0), 0.0, 1.0)
    share = jnp.sum(jnp.sum(share, axis=1, keepdims=True), axis=0, keepdims=True)
    mad = 1.4826 * ((512.0 / BINS) * share)
    pk[...] = row / mad
    madrow = jnp.broadcast_to(mad, (8, 128))

    lane8 = lax.broadcasted_iota(jnp.int32, (8, 128), 1)
    for j in range(8):
        at, off = (OWN * j) // 128, (OWN * j) % 128
        piece = pk[pl.ds(at, 8, stride=3), :]
        if off:
            piece = pltpu.roll(piece, 128 - off, 1)
            if off + OWN > 128:
                nxt = pltpu.roll(pk[pl.ds(at + 1, 8, stride=3), :], 128 - off, 1)
                piece = jnp.where(lane8 < 128 - off, piece, nxt)
        piece = jnp.where(lane8 < OWN, piece, madrow)
        for g in range(8):
            outr[8 * g + j] = piece[g : g + 1, :]

    def copy_o(xx, zz, cc):
        to = xx * 16 + zz * 2 + cc
        return pltpu.make_async_remote_copy(
            src_ref=outr.at[to], dst_ref=got.at[s], send_sem=sem_os, recv_sem=sem_or,
            device_id=(to, tp), device_id_type=MESH)

    def send(k, _):
        zz = place(k)
        for d in (2, 1, 3, 0):
            copy_o(others[d], zz, c).start()
            copy_o(others[d], zz, 1 - c).start()
        return 0

    lax.fori_loop(0, 7, send, 0)
    for d in (2, 1, 3):
        copy_o(others[d], z, c).start()
        copy_o(others[d], z, 1 - c).start()
    copy_o(x, z, 1 - c).start()
    got[s] = outr[s]
    pltpu.make_async_copy(outr.at[pl.ds(0, 63)], got.at[pl.ds(0, 63)], sem_or).wait()

    best = jnp.max(got[...], axis=0)
    pkgot[0] = best

    def copy_p(d):
        return pltpu.make_async_remote_copy(
            src_ref=pkgot.at[0], dst_ref=pkgot.at[d], send_sem=sem_ps.at[d - 1],
            recv_sem=sem_pr.at[d - 1], device_id=(s, (tp + d) % 8), device_id_type=MESH)

    for d in (4, 3, 5, 2, 6, 1, 7):
        copy_p(d).start()
    flat = jnp.concatenate([got[i] for i in range(64)] + [jnp.zeros((64, 128), F32)], axis=0)
    turned = flat.T
    score_ref[...] = turned[0:OWN, 0:NT]
    mad_ref[...] = turned[OWN : OWN + 1, 0:NT]
    for d in (1, 7, 2, 6, 3, 5, 4):
        copy_p(d).wait_recv()
        best = jnp.maximum(best, pkgot[d])
    peak_ref[...] = best[:, 0:OWN]

    for k in range(8):
        copy_c(k).wait_send()
        for d in range(1, 4):
            copy_x(k, d).wait_send()
    for k in range(7):
        copy_z(k).wait_send()
        copy_p(k + 1).wait_send()
    pltpu.make_async_copy(outr.at[pl.ds(0, 63)], got.at[pl.ds(0, 63)], sem_os).wait()


def put_out(a, b, c, a_out, b_out, c_out, sems):
    copies = [
        pltpu.make_async_copy(one, two, sems.at[i])
        for i, (one, two) in enumerate(((a, a_out), (b, b_out), (c, c_out)))
    ]
    for copy in copies:
        copy.start()
    for copy in copies:
        copy.wait()


def on_device(waveform, templates, lags, present):
    vmem = pl.BlockSpec(memory_space=pltpu.VMEM)
    dma = pltpu.SemaphoreType.DMA
    hbm = pl.BlockSpec(memory_space=pltpu.HBM)
    results = pl.pallas_call(
        kernel,
        out_shape=(
            jax.ShapeDtypeStruct((OWN, NT), F32),
            jax.ShapeDtypeStruct((1, NT), F32),
            jax.ShapeDtypeStruct((1, OWN), F32),
        ),
        in_specs=[hbm, hbm, hbm, hbm],
        out_specs=(vmem, vmem, vmem),
        scratch_shapes=[
            pltpu.VMEM((CHANS, SAMPLES), BF16),
            pltpu.VMEM((NT, CHANS * LEN), BF16),
            pltpu.SMEM((1, NT), jnp.int32),
            pltpu.SMEM((1, NT), jnp.int32),
            dma((4,)),
            pltpu.VMEM((8, 53 * 128), F32),
            pltpu.VMEM((NQ * NT, 2 * CHANS * TAPS), BF16),
            pltpu.VMEM((CHANS * TAPS, (CH + 1) * 128), BF16),
            pltpu.VMEM((CHANS * TAPS, (CH + 1) * 128), BF16),
            pltpu.VMEM((CHANS * TAPS, (CH + 1) * 128), BF16),
            pltpu.VMEM((NQ * NT * NBLK, 128), F32),
            pltpu.VMEM((NT, 128), F32),
            pltpu.VMEM((8, 4, ROWS, 128), F32),
            pltpu.VMEM((8, 4, ROWS, 128), F32),
            pltpu.VMEM((8, 4, ROWS, 128), F32),
            pltpu.VMEM((8, 3, ROWS, 128), F32),
            pltpu.VMEM((8, 3, ROWS, 128), F32),
            pltpu.VMEM((7, ROWS, 128), F32),
            pltpu.VMEM((7, ROWS, 128), F32),
            pltpu.VMEM((64, 1, 128), F32),
            pltpu.VMEM((64, 1, 128), F32),
            pltpu.VMEM((ROWS, 128), F32),
            pltpu.VMEM((8, 1, 128), F32),
            dma((8,)), dma((8,)), dma((8, 3)), dma((8, 3)), dma((7,)), dma((7,)),
            dma(()), dma(()), dma((7,)), dma((7,)),
        ],
        compiler_params=pltpu.CompilerParams(
            collective_id=0, has_side_effects=True, vmem_limit_bytes=50 * 1024 * 1024),
    )(
        *(
            pltpu.with_memory_space_constraint(value, pltpu.HBM)
            for value in (
                waveform[0], templates[:, 0, :], lags.reshape(1, NT), present.reshape(1, NT))
        )
    )
    score, mad, peak = pl.pallas_call(
        put_out,
        out_shape=(
            jax.ShapeDtypeStruct((OWN, NT), F32),
            jax.ShapeDtypeStruct((1, NT), F32),
            jax.ShapeDtypeStruct((1, OWN), F32),
        ),
        in_specs=[vmem, vmem, vmem],
        out_specs=(hbm, hbm, hbm),
        scratch_shapes=[dma((3,))],
        compiler_params=pltpu.CompilerParams(vmem_limit_bytes=1024 * 1024),
    )(*results)
    return score, mad[0], peak[0]


def solution(mesh):
    return jax.shard_map(
        on_device,
        mesh=mesh,
        in_specs=(P("sta", None, None), P("tpl", "sta", None), P("tpl", "sta"), P("tpl", "sta")),
        out_specs=(P("sta", "tpl"), P("tpl"), P("sta")),
        check_vma=False,
    )
```

```python
import functools

import jax
import jax.numpy as jnp
from jax import lax
from jax.experimental import pallas as pl
from jax.experimental.pallas import tpu as pltpu
from jax.sharding import PartitionSpec as P

LEN = 512
CHANS = 3
SAMPLES = 6583
BINS = 1024
TOUT = 3072
NT = 64
TAPS = 128
NQ = 2
NBLK = 50
CH = 4
ROWS = TOUT // 128
OWN = TOUT // 64
F32 = jnp.float32
BF16 = jnp.bfloat16
MESH = pl.DeviceIdType.MESH
AWAY = (4, 3, 5, 2, 6, 1, 7, 0)


def kernel(
    wave_hbm, temp_hbm, lag_hbm, pres_hbm, score_ref, mad_ref, peak_ref,
    wave_ref, temp_ref, lag_ref, pres_ref, sem_in, wrow, amat, hank0, hank1, hank2, part, scl, sendc, own, recvc, sendx, recvx, sendz, recvz,
    outr, got, pk, pk1, pkgot,
    sem_cs, sem_cr, sem_xs, sem_xr, sem_zs, sem_zr, sem_os, sem_or, sem_ps, sem_pr,
):
    s = lax.axis_index("sta")
    tp = lax.axis_index("tpl")
    x, z, c = s // 16, (s // 2) % 8, s % 2

    def dev(xx, zz, cc):
        return (xx * 16 + zz * 2 + cc, tp)

    inputs = [
        pltpu.make_async_copy(a, b, sem_in.at[i])
        for i, (a, b) in enumerate(
            ((temp_hbm, temp_ref), (wave_hbm, wave_ref), (lag_hbm, lag_ref), (pres_hbm, pres_ref))
        )
    ]
    for copy in inputs:
        copy.start()

    barrier = pltpu.get_barrier_semaphore()
    for i in (4, 3, 5, 2, 6, 1, 7):
        pl.semaphore_signal(barrier, inc=1, device_id=(s, (tp + i) % 8), device_id_type=MESH)
        pl.semaphore_signal(barrier, inc=1, device_id=dev(x, (z + i) % 8, c), device_id_type=MESH)
    for i in (2, 1, 3):
        pl.semaphore_signal(barrier, inc=1, device_id=dev((x + i) % 4, z, c), device_id_type=MESH)
    pl.semaphore_signal(barrier, inc=1, device_id=dev(x, z, 1 - c), device_id_type=MESH)

    wrow[...] = jnp.zeros(wrow.shape, F32)
    inputs[1].wait()
    wrow[0:CHANS, 0:SAMPLES] = wave_ref[...].astype(F32)

    rho = lax.broadcasted_iota(jnp.int32, (16, 128), 0)
    lane16 = lax.broadcasted_iota(jnp.int32, (16, 128), 1)

    def build(j, into, ahead=None):
        for ch in range(CHANS):
            for g in range(TAPS // 16):
                rows = slice(ch * TAPS + g * 16, ch * TAPS + (g + 1) * 16)
                first = lane16 <= rho + 16 * g
                before = None
                for b in range(CH + 1):
                    at = pl.multiple_of((j * CH + b) * 128, 128)
                    row = jnp.broadcast_to(wrow[ch : ch + 1, pl.ds(at, 128)], (16, 128))
                    after = pltpu.roll(row, 1 + 16 * g, 1, stride=1, stride_axis=0)
                    if b:
                        block = jnp.where(first, before, after).astype(BF16)
                        into[rows, (b - 1) * 128 : b * 128] = block
                        if b == 1 and ahead is not None:
                            ahead[rows, CH * 128 : (CH + 1) * 128] = block
                    before = after

    def multiply(j, held, tiles=CH // 2):
        for p in range(tiles):
            halves = []
            for ch in range(CHANS):
                for h in range(2):
                    at = (2 * p + h) * 128
                    halves.append(held[ch * TAPS : (ch + 1) * TAPS, at : at + 256])
            out = jnp.dot(
                amat[...], jnp.concatenate(halves, axis=0), preferred_element_type=F32)
            for g in range(NQ * NT // 8):
                for b in range(2):
                    part[pl.ds(g * 8 * NBLK + j * CH + 2 * p + b, 8, stride=NBLK), :] = out[
                        g * 8 : (g + 1) * 8, b * 128 : (b + 1) * 128
                    ]

    def chunks(i, _):
        multiply(3 * i, hank0)
        build(3 * i + 2, hank2, hank1)
        multiply(3 * i + 1, hank1)
        build(3 * i + 3, hank0, hank2)
        multiply(3 * i + 2, hank2)
        build(3 * i + 4, hank1, hank0)
        return 0

    build(0, hank0)
    build(1, hank1, hank0)
    inputs[0].wait()
    inputs[2].wait()
    inputs[3].wait()

    total = jnp.zeros((NT, 128), F32)
    flip_i = lax.broadcasted_iota(jnp.int32, (128, 128), 0)
    flip_j = lax.broadcasted_iota(jnp.int32, (128, 128), 1)
    flip = jnp.where(flip_i + flip_j == 127, 1.0, 0.0).astype(BF16)
    for ch in range(CHANS):
        for k in range(LEN // TAPS):
            piece = temp_ref[:, ch * LEN + k * TAPS : ch * LEN + (k + 1) * TAPS]
            wide = piece.astype(F32)
            total = total + wide * wide
            turned = jnp.dot(piece, flip, preferred_element_type=F32).astype(BF16)
            at = (ch * 2 + k % 2) * TAPS
            amat[(k // 2) * NT : (k // 2 + 1) * NT, at : at + TAPS] = turned
    norm = jnp.sqrt(jnp.sum(total, axis=1, keepdims=True) + 1e-6)
    scl[...] = jnp.broadcast_to(1.0 / norm, (NT, 128))
    lax.fori_loop(0, 3, chunks, 0)
    multiply(9, hank0)
    build(11, hank2, hank1)
    multiply(10, hank1)
    build(12, hank0, hank2)
    multiply(11, hank2)
    multiply(12, hank0, 1)

    lane24 = lax.broadcasted_iota(jnp.int32, (ROWS, 128), 1)

    def shifted(t):
        lag = lag_ref[0, t]
        here = pres_ref[0, t].astype(F32)
        a, r = lax.shift_right_logical(lag, 7), lax.bitwise_and(lag, 127)
        left = right = None
        for q in range(NQ):
            at = (q * NT + t) * NBLK + 2 * q + a
            one, two = part[pl.ds(at, ROWS), :], part[pl.ds(at + 1, ROWS), :]
            left = one if left is None else left + one
            right = two if right is None else right + two
        by = lax.bitwise_and(128 - r, 127)
        left, right = pltpu.roll(left, by, 1), pltpu.roll(right, by, 1)
        return jnp.where(lane24 < 128 - r, left, right) * (scl[pl.ds(t, 1), :] * here)

    def place(k):
        return (z + 4 + k // 2 - (k % 2) * k + 8) % 8

    beyond = [(z + AWAY[k]) % 8 for k in range(8)]
    others = [(x + d) % 4 for d in range(4)]
    group = [others[d] * 16 for d in range(4)]

    def copy_c(k):
        return pltpu.make_async_remote_copy(
            src_ref=sendc.at[k], dst_ref=recvc.at[k], send_sem=sem_cs, recv_sem=sem_cr.at[k],
            device_id=dev(x, z, 1 - c), device_id_type=MESH)

    def copy_x(k, d):
        return pltpu.make_async_remote_copy(
            src_ref=sendx.at[k, d - 1], dst_ref=recvx.at[k, d - 1],
            send_sem=sem_xs, recv_sem=sem_xr.at[k],
            device_id=dev(others[d], z, c), device_id_type=MESH)

    def copy_z(k):
        return pltpu.make_async_remote_copy(
            src_ref=sendz.at[k], dst_ref=recvz.at[k], send_sem=sem_zs, recv_sem=sem_zr,
            device_id=dev(x, beyond[k], c), device_id_type=MESH)

    def both(k):
        at = beyond[k] * 2
        for d in range(4):
            sendc[k, d] = shifted(group[d] + at + 1 - c)
        copy_c(k).start()
        for d in range(4):
            own[k, d] = shifted(group[d] + at + c)

    def fold(k):
        copy_c(k).wait_recv()
        for d in (2, 1, 3):
            sendx[k, d - 1] = own[k, d] + recvc[k, d]
            copy_x(k, d).start()

    def reduced(k):
        pltpu.make_async_copy(sendx.at[k], recvx.at[k], sem_xr.at[k]).wait()
        total = (own[k, 0] + recvc[k, 0]) + (recvx[k, 0] + recvx[k, 1] + recvx[k, 2])
        if k < 7:
            sendz[k] = total
            copy_z(k).start()
        return total

    pl.semaphore_wait(barrier, 1 + 3 + 7 + 7)
    for k in range(8):
        both(k)
        if k >= 5:
            fold(k - 5)
    for k in range(3, 8):
        fold(k)
    for k in range(7):
        reduced(k)
    row = reduced(7)
    pltpu.make_async_copy(sendz, recvz, sem_zr).wait()
    for k in range(7):
        row = row + recvz[k]

    pos = jnp.clip(jnp.abs(row) * (BINS / 512.0) - 0.5, 0.0, BINS - 1.0)
    low = jnp.minimum(jnp.floor(pos), BINS - 2.0)
    high = jnp.floor(low * (1.0 / 32.0))
    inside = pos - 32.0 * high
    iota_h = lax.broadcasted_iota(jnp.int32, (32, 128), 0).astype(F32)
    iota_l = lax.broadcasted_iota(jnp.int32, (40, 128), 0).astype(F32)
    ones, hats = [], [[], [], []]
    for i in range(ROWS):
        ones.append(jnp.where(iota_h == high[i : i + 1, :], 1.0, 0.0).astype(BF16))
        hat = jnp.maximum(1.0 - jnp.abs(inside[i : i + 1, :] - iota_l), 0.0)
        for k in range(3):
            near = hat.astype(BF16)
            hats[k].append(near)
            hat = hat - near.astype(F32)
    ones = jnp.concatenate(ones, axis=1)
    stacked = jnp.concatenate([jnp.concatenate(piece, axis=1) for piece in hats], axis=0)
    counts = lax.dot_general(stacked, ones, (((1,), (1,)), ((), ())), preferred_element_type=F32)
    counts = counts[0:40, :] + counts[40:80, :] + counts[80:120, :]
    over = jnp.concatenate([jnp.zeros((1, 1), F32), counts[32:33, 0:31]], axis=1)
    row_l = lax.broadcasted_iota(jnp.int32, (32, 32), 0)
    col_h = lax.broadcasted_iota(jnp.int32, (32, 32), 1)
    below = jnp.where(col_h < row_l, 1.0, 0.0)
    above = jnp.where(row_l < col_h, 1.0, 0.0)
    sums = jnp.broadcast_to(jnp.sum(counts, axis=0, keepdims=True), (8, 32))
    before = jnp.dot(
        below, counts[0:32, :], precision=lax.Precision.HIGHEST, preferred_element_type=F32)
    before = before + jnp.dot(
        sums, above, precision=lax.Precision.HIGHEST, preferred_element_type=F32)[0:1, :]
    over = jnp.where(row_l == 0, jnp.broadcast_to(over, (32, 32)), 0.0)
    before = before - over
    counts = counts[0:32, :] + over
    share = jnp.clip((0.5 * TOUT - before) / jnp.maximum(counts, 1.0), 0.0, 1.0)
    share = jnp.sum(jnp.sum(share, axis=0, keepdims=True), axis=1, keepdims=True)
    mad = 1.4826 * ((512.0 / BINS) * share)
    pk[...] = row / mad
    madrow = jnp.broadcast_to(mad, (8, 128))

    lane8 = lax.broadcasted_iota(jnp.int32, (8, 128), 1)
    for j in range(8):
        at, off = (OWN * j) // 128, (OWN * j) % 128
        piece = pk[pl.ds(at, 8, stride=3), :]
        if off:
            piece = pltpu.roll(piece, 128 - off, 1)
            if off + OWN > 128:
                nxt = pltpu.roll(pk[pl.ds(at + 1, 8, stride=3), :], 128 - off, 1)
                piece = jnp.where(lane8 < 128 - off, piece, nxt)
        piece = jnp.where(lane8 < OWN, piece, madrow)
        for g in range(8):
            outr[8 * g + j] = piece[g : g + 1, :]

    def copy_o(xx, zz, cc):
        to = xx * 16 + zz * 2 + cc
        return pltpu.make_async_remote_copy(
            src_ref=outr.at[to], dst_ref=got.at[s], send_sem=sem_os, recv_sem=sem_or,
            device_id=(to, tp), device_id_type=MESH)

    def send(k, _):
        zz = place(k)
        for d in (2, 1, 3, 0):
            copy_o(others[d], zz, c).start()
            copy_o(others[d], zz, 1 - c).start()
        return 0

    lax.fori_loop(0, 7, send, 0)
    for d in (2, 1, 3):
        copy_o(others[d], z, c).start()
        copy_o(others[d], z, 1 - c).start()
    copy_o(x, z, 1 - c).start()
    got[s] = outr[s]
    pltpu.make_async_copy(outr.at[pl.ds(0, 63)], got.at[pl.ds(0, 63)], sem_or).wait()

    best = jnp.max(got[...], axis=0)
    pk1[...] = best

    def copy_p(d):
        return pltpu.make_async_remote_copy(
            src_ref=pk1, dst_ref=pkgot.at[d - 1], send_sem=sem_ps, recv_sem=sem_pr, device_id=(s, (tp + d) % 8), device_id_type=MESH)

    for d in (4, 3, 5, 2, 6, 1, 7):
        copy_p(d).start()
    flat = jnp.concatenate([got[i] for i in range(64)] + [jnp.zeros((64, 128), F32)], axis=0)
    turned = flat.T
    score_ref[...] = turned[0:OWN, 0:NT]
    mad_ref[...] = turned[OWN : OWN + 1, 0:NT]
    pltpu.make_async_copy(pkgot, pkgot, sem_pr).wait()
    for d in range(7):
        best = jnp.maximum(best, pkgot[d])
    peak_ref[...] = best[:, 0:OWN]

    pltpu.make_async_copy(sendc, recvc, sem_cs).wait()
    pltpu.make_async_copy(sendx, recvx, sem_xs).wait()
    pltpu.make_async_copy(sendz, recvz, sem_zs).wait()
    pltpu.make_async_copy(pkgot, pkgot, sem_ps).wait()
    pltpu.make_async_copy(outr.at[pl.ds(0, 63)], got.at[pl.ds(0, 63)], sem_os).wait()


def put_out(a, b, c, a_out, b_out, c_out, sems):
    copies = [
        pltpu.make_async_copy(one, two, sems.at[i])
        for i, (one, two) in enumerate(((a, a_out), (b, b_out), (c, c_out)))
    ]
    for copy in copies:
        copy.start()
    for copy in copies:
        copy.wait()


def on_device(waveform, templates, lags, present):
    vmem = pl.BlockSpec(memory_space=pltpu.VMEM)
    dma = pltpu.SemaphoreType.DMA
    hbm = pl.BlockSpec(memory_space=pltpu.HBM)
    results = pl.pallas_call(
        kernel,
        out_shape=(
            jax.ShapeDtypeStruct((OWN, NT), F32),
            jax.ShapeDtypeStruct((1, NT), F32),
            jax.ShapeDtypeStruct((1, OWN), F32),
        ),
        in_specs=[hbm, hbm, hbm, hbm],
        out_specs=(vmem, vmem, vmem),
        scratch_shapes=[
            pltpu.VMEM((CHANS, SAMPLES), BF16),
            pltpu.VMEM((NT, CHANS * LEN), BF16),
            pltpu.SMEM((1, NT), jnp.int32),
            pltpu.SMEM((1, NT), jnp.int32),
            dma((4,)),
            pltpu.VMEM((8, 53 * 128), F32),
            pltpu.VMEM((NQ * NT, 2 * CHANS * TAPS), BF16),
            pltpu.VMEM((CHANS * TAPS, (CH + 1) * 128), BF16),
            pltpu.VMEM((CHANS * TAPS, (CH + 1) * 128), BF16),
            pltpu.VMEM((CHANS * TAPS, (CH + 1) * 128), BF16),
            pltpu.VMEM((NQ * NT * NBLK, 128), F32),
            pltpu.VMEM((NT, 128), F32),
            pltpu.VMEM((8, 4, ROWS, 128), F32),
            pltpu.VMEM((8, 4, ROWS, 128), F32),
            pltpu.VMEM((8, 4, ROWS, 128), F32),
            pltpu.VMEM((8, 3, ROWS, 128), F32),
            pltpu.VMEM((8, 3, ROWS, 128), F32),
            pltpu.VMEM((7, ROWS, 128), F32),
            pltpu.VMEM((7, ROWS, 128), F32),
            pltpu.VMEM((64, 1, 128), F32),
            pltpu.VMEM((64, 1, 128), F32),
            pltpu.VMEM((ROWS, 128), F32),
            pltpu.VMEM((1, 128), F32),
            pltpu.VMEM((7, 1, 128), F32),
            dma(()), dma((8,)), dma(()), dma((8,)), dma(()), dma(()),
            dma(()), dma(()), dma(()), dma(()),
        ],
        compiler_params=pltpu.CompilerParams(
            collective_id=0, has_side_effects=True, vmem_limit_bytes=50 * 1024 * 1024),
    )(
        *(
            pltpu.with_memory_space_constraint(value, pltpu.HBM)
            for value in (
                waveform[0], templates[:, 0, :], lags.reshape(1, NT), present.reshape(1, NT))
        )
    )
    score, mad, peak = pl.pallas_call(
        put_out,
        out_shape=(
            jax.ShapeDtypeStruct((OWN, NT), F32),
            jax.ShapeDtypeStruct((1, NT), F32),
            jax.ShapeDtypeStruct((1, OWN), F32),
        ),
        in_specs=[vmem, vmem, vmem],
        out_specs=(hbm, hbm, hbm),
        scratch_shapes=[dma((3,))],
        compiler_params=pltpu.CompilerParams(vmem_limit_bytes=1024 * 1024),
    )(*results)
    return score, mad[0], peak[0]


def solution(mesh):
    return jax.shard_map(
        on_device,
        mesh=mesh,
        in_specs=(P("sta", None, None), P("tpl", "sta", None), P("tpl", "sta"), P("tpl", "sta")),
        out_specs=(P("sta", "tpl"), P("tpl"), P("sta")),
        check_vma=False,
    )
```

```python
import functools

import jax
import jax.numpy as jnp
from jax import lax
from jax.experimental import pallas as pl
from jax.experimental.pallas import tpu as pltpu
from jax.sharding import PartitionSpec as P

LEN = 512
CHANS = 3
SAMPLES = 6583
BINS = 1024
TOUT = 3072
NT = 64
TAPS = 128
NQ = 2
NBLK = 50
CH = 4
ROWS = TOUT // 128
OWN = TOUT // 64
F32 = jnp.float32
BF16 = jnp.bfloat16
MESH = pl.DeviceIdType.MESH
AWAY = (4, 3, 5, 2, 6, 1, 7, 0)


def kernel(
    wave_hbm, temp_hbm, lag_hbm, pres_hbm, score_ref, mad_ref, peak_ref,
    wave_ref, temp_ref, lag_ref, pres_ref, sem_in, wrow, amat, hank0, hank1, hank2, last0, last1, last2, part, scl, sendc, own, recvc, sendx, recvx, sendz, recvz,
    outr, got, pk, pk1, pkgot,
    sem_cs, sem_cr, sem_xs, sem_xr, sem_zs, sem_zr, sem_os, sem_or, sem_ps, sem_pr,
):
    s = lax.axis_index("sta")
    tp = lax.axis_index("tpl")
    x, z, c = s // 16, (s // 2) % 8, s % 2

    def dev(xx, zz, cc):
        return (xx * 16 + zz * 2 + cc, tp)

    inputs = [
        pltpu.make_async_copy(a, b, sem_in.at[i])
        for i, (a, b) in enumerate(
            ((temp_hbm, temp_ref), (wave_hbm, wave_ref), (lag_hbm, lag_ref), (pres_hbm, pres_ref))
        )
    ]
    for copy in inputs:
        copy.start()

    barrier = pltpu.get_barrier_semaphore()
    for i in (4, 3, 5, 2, 6, 1, 7):
        pl.semaphore_signal(barrier, inc=1, device_id=(s, (tp + i) % 8), device_id_type=MESH)
        pl.semaphore_signal(barrier, inc=1, device_id=dev(x, (z + i) % 8, c), device_id_type=MESH)
    for i in (2, 1, 3):
        pl.semaphore_signal(barrier, inc=1, device_id=dev((x + i) % 4, z, c), device_id_type=MESH)
    pl.semaphore_signal(barrier, inc=1, device_id=dev(x, z, 1 - c), device_id_type=MESH)

    wrow[...] = jnp.zeros(wrow.shape, F32)
    inputs[1].wait()
    wrow[0:CHANS, 0:SAMPLES] = wave_ref[...].astype(F32)

    rho = lax.broadcasted_iota(jnp.int32, (16, 128), 0)
    lane16 = lax.broadcasted_iota(jnp.int32, (16, 128), 1)

    def build(j, into, ahead=None, old=None, new=None):
        for ch in range(CHANS):
            for g in range(TAPS // 16):
                rows = slice(ch * TAPS + g * 16, ch * TAPS + (g + 1) * 16)
                first = lane16 <= rho + 16 * g
                before = None if old is None else old[rows, :].astype(F32)
                for b in range(0 if old is None else 1, CH + 1):
                    at = pl.multiple_of((j * CH + b) * 128, 128)
                    row = jnp.broadcast_to(wrow[ch : ch + 1, pl.ds(at, 128)], (16, 128))
                    after = pltpu.roll(row, 1 + 16 * g, 1, stride=1, stride_axis=0)
                    if b:
                        block = jnp.where(first, before, after).astype(BF16)
                        into[rows, (b - 1) * 128 : b * 128] = block
                        if b == 1 and ahead is not None:
                            ahead[rows, CH * 128 : (CH + 1) * 128] = block
                    before = after
                if new is not None:
                    new[rows, :] = before.astype(BF16)

    def multiply(j, held, tiles=CH // 2):
        for p in range(tiles):
            halves = []
            for ch in range(CHANS):
                for h in range(2):
                    at = (2 * p + h) * 128
                    halves.append(held[ch * TAPS : (ch + 1) * TAPS, at : at + 256])
            out = jnp.dot(
                amat[...], jnp.concatenate(halves, axis=0), preferred_element_type=F32)
            for g in range(NQ * NT // 8):
                for b in range(2):
                    part[pl.ds(g * 8 * NBLK + j * CH + 2 * p + b, 8, stride=NBLK), :] = out[
                        g * 8 : (g + 1) * 8, b * 128 : (b + 1) * 128
                    ]

    def chunks(i, _):
        multiply(3 * i, hank0)
        build(3 * i + 2, hank2, hank1, last1, last2)
        multiply(3 * i + 1, hank1)
        build(3 * i + 3, hank0, hank2, last2, last0)
        multiply(3 * i + 2, hank2)
        build(3 * i + 4, hank1, hank0, last0, last1)
        return 0

    build(0, hank0, None, None, last0)
    build(1, hank1, hank0, last0, last1)
    inputs[0].wait()
    inputs[2].wait()
    inputs[3].wait()

    total = jnp.zeros((NT, 128), F32)
    flip_i = lax.broadcasted_iota(jnp.int32, (128, 128), 0)
    flip_j = lax.broadcasted_iota(jnp.int32, (128, 128), 1)
    flip = jnp.where(flip_i + flip_j == 127, 1.0, 0.0).astype(BF16)
    for ch in range(CHANS):
        for k in range(LEN // TAPS):
            piece = temp_ref[:, ch * LEN + k * TAPS : ch * LEN + (k + 1) * TAPS]
            wide = piece.astype(F32)
            total = total + wide * wide
            turned = jnp.dot(piece, flip, preferred_element_type=F32).astype(BF16)
            at = (ch * 2 + k % 2) * TAPS
            amat[(k // 2) * NT : (k // 2 + 1) * NT, at : at + TAPS] = turned
    norm = jnp.sqrt(jnp.sum(total, axis=1, keepdims=True) + 1e-6)
    scl[...] = jnp.broadcast_to(1.0 / norm, (NT, 128))
    lax.fori_loop(0, 3, chunks, 0)
    multiply(9, hank0)
    build(11, hank2, hank1, last1, last2)
    multiply(10, hank1)
    build(12, hank0, hank2, last2)
    multiply(11, hank2)
    multiply(12, hank0, 1)

    lane24 = lax.broadcasted_iota(jnp.int32, (ROWS, 128), 1)

    def shifted(t):
        lag = lag_ref[0, t]
        here = pres_ref[0, t].astype(F32)
        a, r = lax.shift_right_logical(lag, 7), lax.bitwise_and(lag, 127)
        left = right = None
        for q in range(NQ):
            at = (q * NT + t) * NBLK + 2 * q + a
            one, two = part[pl.ds(at, ROWS), :], part[pl.ds(at + 1, ROWS), :]
            left = one if left is None else left + one
            right = two if right is None else right + two
        by = lax.bitwise_and(128 - r, 127)
        left, right = pltpu.roll(left, by, 1), pltpu.roll(right, by, 1)
        return jnp.where(lane24 < 128 - r, left, right) * (scl[pl.ds(t, 1), :] * here)

    def place(k):
        return (z + 4 + k // 2 - (k % 2) * k + 8) % 8

    beyond = [(z + AWAY[k]) % 8 for k in range(8)]
    others = [(x + d) % 4 for d in range(4)]
    group = [others[d] * 16 for d in range(4)]

    def copy_c(k):
        return pltpu.make_async_remote_copy(
            src_ref=sendc.at[k], dst_ref=recvc.at[k], send_sem=sem_cs, recv_sem=sem_cr.at[k],
            device_id=dev(x, z, 1 - c), device_id_type=MESH)

    def copy_x(k, d):
        return pltpu.make_async_remote_copy(
            src_ref=sendx.at[k, d - 1], dst_ref=recvx.at[k, d - 1],
            send_sem=sem_xs, recv_sem=sem_xr.at[k],
            device_id=dev(others[d], z, c), device_id_type=MESH)

    def copy_z(k):
        return pltpu.make_async_remote_copy(
            src_ref=sendz.at[k], dst_ref=recvz.at[k], send_sem=sem_zs, recv_sem=sem_zr,
            device_id=dev(x, beyond[k], c), device_id_type=MESH)

    def both(k):
        at = beyond[k] * 2
        for d in range(4):
            sendc[k, d] = shifted(group[d] + at + 1 - c)
        copy_c(k).start()
        for d in range(4):
            own[k, d] = shifted(group[d] + at + c)

    def fold(k):
        copy_c(k).wait_recv()
        for d in (2, 1, 3):
            sendx[k, d - 1] = own[k, d] + recvc[k, d]
            copy_x(k, d).start()

    def reduced(k):
        pltpu.make_async_copy(sendx.at[k], recvx.at[k], sem_xr.at[k]).wait()
        total = (own[k, 0] + recvc[k, 0]) + (recvx[k, 0] + recvx[k, 1] + recvx[k, 2])
        if k < 7:
            sendz[k] = total
            copy_z(k).start()
        return total

    pl.semaphore_wait(barrier, 1 + 3 + 7 + 7)
    for k in range(8):
        both(k)
        if k >= 5:
            fold(k - 5)
    for k in range(3, 8):
        fold(k)
    for k in range(7):
        reduced(k)
    row = reduced(7)
    pltpu.make_async_copy(sendz, recvz, sem_zr).wait()
    for k in range(7):
        row = row + recvz[k]

    pos = jnp.clip(jnp.abs(row) * (BINS / 512.0) - 0.5, 0.0, BINS - 1.0)
    low = jnp.minimum(jnp.floor(pos), BINS - 2.0)
    high = jnp.floor(low * (1.0 / 32.0))
    inside = pos - 32.0 * high
    iota_h = lax.broadcasted_iota(jnp.int32, (32, 128), 0).astype(F32)
    iota_l = lax.broadcasted_iota(jnp.int32, (40, 128), 0).astype(F32)
    ones, hats = [], [[], [], []]
    for i in range(ROWS):
        ones.append(jnp.where(iota_h == high[i : i + 1, :], 1.0, 0.0).astype(BF16))
        hat = jnp.maximum(1.0 - jnp.abs(inside[i : i + 1, :] - iota_l), 0.0)
        for k in range(3):
            near = hat.astype(BF16)
            hats[k].append(near)
            hat = hat - near.astype(F32)
    ones = jnp.concatenate(ones, axis=1)
    stacked = jnp.concatenate([jnp.concatenate(piece, axis=1) for piece in hats], axis=0)
    counts = lax.dot_general(stacked, ones, (((1,), (1,)), ((), ())), preferred_element_type=F32)
    counts = counts[0:40, :] + counts[40:80, :] + counts[80:120, :]
    over = jnp.concatenate([jnp.zeros((1, 1), F32), counts[32:33, 0:31]], axis=1)
    row_l = lax.broadcasted_iota(jnp.int32, (32, 32), 0)
    col_h = lax.broadcasted_iota(jnp.int32, (32, 32), 1)
    below = jnp.where(col_h < row_l, 1.0, 0.0)
    above = jnp.where(row_l < col_h, 1.0, 0.0)
    sums = jnp.broadcast_to(jnp.sum(counts, axis=0, keepdims=True), (8, 32))
    before = jnp.dot(
        below, counts[0:32, :], precision=lax.Precision.HIGHEST, preferred_element_type=F32)
    before = before + jnp.dot(
        sums, above, precision=lax.Precision.HIGHEST, preferred_element_type=F32)[0:1, :]
    over = jnp.where(row_l == 0, jnp.broadcast_to(over, (32, 32)), 0.0)
    before = before - over
    counts = counts[0:32, :] + over
    share = jnp.clip((0.5 * TOUT - before) / jnp.maximum(counts, 1.0), 0.0, 1.0)
    share = jnp.sum(jnp.sum(share, axis=0, keepdims=True), axis=1, keepdims=True)
    mad = 1.4826 * ((512.0 / BINS) * share)
    pk[...] = row / mad
    madrow = jnp.broadcast_to(mad, (8, 128))

    lane8 = lax.broadcasted_iota(jnp.int32, (8, 128), 1)
    for j in range(8):
        at, off = (OWN * j) // 128, (OWN * j) % 128
        piece = pk[pl.ds(at, 8, stride=3), :]
        if off:
            piece = pltpu.roll(piece, 128 - off, 1)
            if off + OWN > 128:
                nxt = pltpu.roll(pk[pl.ds(at + 1, 8, stride=3), :], 128 - off, 1)
                piece = jnp.where(lane8 < 128 - off, piece, nxt)
        piece = jnp.where(lane8 < OWN, piece, madrow)
        for g in range(8):
            outr[8 * g + j] = piece[g : g + 1, :]

    def copy_o(xx, zz, cc):
        to = xx * 16 + zz * 2 + cc
        return pltpu.make_async_remote_copy(
            src_ref=outr.at[to], dst_ref=got.at[s], send_sem=sem_os, recv_sem=sem_or,
            device_id=(to, tp), device_id_type=MESH)

    def send(k, _):
        zz = place(k)
        for d in (2, 1, 3, 0):
            copy_o(others[d], zz, c).start()
            copy_o(others[d], zz, 1 - c).start()
        return 0

    lax.fori_loop(0, 7, send, 0)
    for d in (2, 1, 3):
        copy_o(others[d], z, c).start()
        copy_o(others[d], z, 1 - c).start()
    copy_o(x, z, 1 - c).start()
    got[s] = outr[s]
    pltpu.make_async_copy(outr.at[pl.ds(0, 63)], got.at[pl.ds(0, 63)], sem_or).wait()

    best = jnp.max(got[...], axis=0)
    pk1[...] = best

    def copy_p(d):
        return pltpu.make_async_remote_copy(
            src_ref=pk1, dst_ref=pkgot.at[d - 1], send_sem=sem_ps, recv_sem=sem_pr, device_id=(s, (tp + d) % 8), device_id_type=MESH)

    for d in (4, 3, 5, 2, 6, 1, 7):
        copy_p(d).start()
    flat = jnp.concatenate([got[i] for i in range(64)] + [jnp.zeros((64, 128), F32)], axis=0)
    turned = flat.T
    score_ref[...] = turned[0:OWN, 0:NT]
    mad_ref[...] = turned[OWN : OWN + 1, 0:NT]
    pltpu.make_async_copy(pkgot, pkgot, sem_pr).wait()
    for d in range(7):
        best = jnp.maximum(best, pkgot[d])
    peak_ref[...] = best[:, 0:OWN]

    pltpu.make_async_copy(sendc, recvc, sem_cs).wait()
    pltpu.make_async_copy(sendx, recvx, sem_xs).wait()
    pltpu.make_async_copy(sendz, recvz, sem_zs).wait()
    pltpu.make_async_copy(pkgot, pkgot, sem_ps).wait()
    pltpu.make_async_copy(outr.at[pl.ds(0, 63)], got.at[pl.ds(0, 63)], sem_os).wait()


def put_out(a, b, c, a_out, b_out, c_out, sems):
    copies = [
        pltpu.make_async_copy(one, two, sems.at[i])
        for i, (one, two) in enumerate(((a, a_out), (b, b_out), (c, c_out)))
    ]
    for copy in copies:
        copy.start()
    for copy in copies:
        copy.wait()


def on_device(waveform, templates, lags, present):
    vmem = pl.BlockSpec(memory_space=pltpu.VMEM)
    dma = pltpu.SemaphoreType.DMA
    hbm = pl.BlockSpec(memory_space=pltpu.HBM)
    results = pl.pallas_call(
        kernel,
        out_shape=(
            jax.ShapeDtypeStruct((OWN, NT), F32),
            jax.ShapeDtypeStruct((1, NT), F32),
            jax.ShapeDtypeStruct((1, OWN), F32),
        ),
        in_specs=[hbm, hbm, hbm, hbm],
        out_specs=(vmem, vmem, vmem),
        scratch_shapes=[
            pltpu.VMEM((CHANS, SAMPLES), BF16),
            pltpu.VMEM((NT, CHANS * LEN), BF16),
            pltpu.SMEM((1, NT), jnp.int32),
            pltpu.SMEM((1, NT), jnp.int32),
            dma((4,)),
            pltpu.VMEM((8, 53 * 128), F32),
            pltpu.VMEM((NQ * NT, 2 * CHANS * TAPS), BF16),
            pltpu.VMEM((CHANS * TAPS, (CH + 1) * 128), BF16),
            pltpu.VMEM((CHANS * TAPS, (CH + 1) * 128), BF16),
            pltpu.VMEM((CHANS * TAPS, (CH + 1) * 128), BF16),
            pltpu.VMEM((CHANS * TAPS, 128), BF16),
            pltpu.VMEM((CHANS * TAPS, 128), BF16),
            pltpu.VMEM((CHANS * TAPS, 128), BF16),
            pltpu.VMEM((NQ * NT * NBLK, 128), F32),
            pltpu.VMEM((NT, 128), F32),
            pltpu.VMEM((8, 4, ROWS, 128), F32),
            pltpu.VMEM((8, 4, ROWS, 128), F32),
            pltpu.VMEM((8, 4, ROWS, 128), F32),
            pltpu.VMEM((8, 3, ROWS, 128), F32),
            pltpu.VMEM((8, 3, ROWS, 128), F32),
            pltpu.VMEM((7, ROWS, 128), F32),
            pltpu.VMEM((7, ROWS, 128), F32),
            pltpu.VMEM((64, 1, 128), F32),
            pltpu.VMEM((64, 1, 128), F32),
            pltpu.VMEM((ROWS, 128), F32),
            pltpu.VMEM((1, 128), F32),
            pltpu.VMEM((7, 1, 128), F32),
            dma(()), dma((8,)), dma(()), dma((8,)), dma(()), dma(()),
            dma(()), dma(()), dma(()), dma(()),
        ],
        compiler_params=pltpu.CompilerParams(
            collective_id=0, has_side_effects=True, vmem_limit_bytes=50 * 1024 * 1024),
    )(
        *(
            pltpu.with_memory_space_constraint(value, pltpu.HBM)
            for value in (
                waveform[0], templates[:, 0, :], lags.reshape(1, NT), present.reshape(1, NT))
        )
    )
    score, mad, peak = pl.pallas_call(
        put_out,
        out_shape=(
            jax.ShapeDtypeStruct((OWN, NT), F32),
            jax.ShapeDtypeStruct((1, NT), F32),
            jax.ShapeDtypeStruct((1, OWN), F32),
        ),
        in_specs=[vmem, vmem, vmem],
        out_specs=(hbm, hbm, hbm),
        scratch_shapes=[dma((3,))],
        compiler_params=pltpu.CompilerParams(vmem_limit_bytes=1024 * 1024),
    )(*results)
    return score, mad[0], peak[0]


def solution(mesh):
    return jax.shard_map(
        on_device,
        mesh=mesh,
        in_specs=(P("sta", None, None), P("tpl", "sta", None), P("tpl", "sta"), P("tpl", "sta")),
        out_specs=(P("sta", "tpl"), P("tpl"), P("sta")),
        check_vma=False,
    )
```

```python
import functools

import jax
import jax.numpy as jnp
from jax import lax
from jax.experimental import pallas as pl
from jax.experimental.pallas import tpu as pltpu
from jax.sharding import PartitionSpec as P

LEN = 512
CHANS = 3
SAMPLES = 6583
BINS = 1024
TOUT = 3072
NT = 64
TAPS = 128
NQ = 2
NBLK = 50
CH = 4
ROWS = TOUT // 128
OWN = TOUT // 64
F32 = jnp.float32
BF16 = jnp.bfloat16
MESH = pl.DeviceIdType.MESH
AWAY = (4, 3, 5, 2, 6, 1, 7, 0)


def kernel(
    wave_hbm, temp_hbm, lag_hbm, pres_hbm, score_ref, mad_ref, peak_ref,
    wave_ref, temp_ref, lag_ref, pres_ref, sem_in, wrow, amat, hank0, hank1, hank2, last0, last1, last2, part, scl, sendc, own, recvc, sendx, recvx, sendz, recvz,
    outr, got, pk, pk1, pkgot,
    sem_cs, sem_cr, sem_xs, sem_xr, sem_zs, sem_zr, sem_os, sem_or, sem_ps, sem_pr,
):
    s = lax.axis_index("sta")
    tp = lax.axis_index("tpl")
    x, z, c = s // 16, (s // 2) % 8, s % 2

    def dev(xx, zz, cc):
        return (xx * 16 + zz * 2 + cc, tp)

    inputs = [
        pltpu.make_async_copy(a, b, sem_in.at[i])
        for i, (a, b) in enumerate(
            ((temp_hbm, temp_ref), (wave_hbm, wave_ref), (lag_hbm, lag_ref), (pres_hbm, pres_ref))
        )
    ]
    for copy in inputs:
        copy.start()

    barrier = pltpu.get_barrier_semaphore()
    for i in (4, 3, 5, 2, 6, 1, 7):
        pl.semaphore_signal(barrier, inc=1, device_id=(s, (tp + i) % 8), device_id_type=MESH)
        pl.semaphore_signal(barrier, inc=1, device_id=dev(x, (z + i) % 8, c), device_id_type=MESH)
    for i in (2, 1, 3):
        pl.semaphore_signal(barrier, inc=1, device_id=dev((x + i) % 4, z, c), device_id_type=MESH)
    pl.semaphore_signal(barrier, inc=1, device_id=dev(x, z, 1 - c), device_id_type=MESH)

    wrow[...] = jnp.zeros(wrow.shape, F32)
    inputs[1].wait()
    wrow[0:CHANS, 0:SAMPLES] = wave_ref[...].astype(F32)

    rho = lax.broadcasted_iota(jnp.int32, (16, 128), 0)
    lane16 = lax.broadcasted_iota(jnp.int32, (16, 128), 1)

    def build(j, into, ahead=None, old=None, new=None):
        for ch in range(CHANS):
            for g in range(TAPS // 16):
                rows = slice(ch * TAPS + g * 16, ch * TAPS + (g + 1) * 16)
                first = lane16 <= rho + 16 * g
                before = None if old is None else old[rows, :].astype(F32)
                for b in range(0 if old is None else 1, CH + 1):
                    at = pl.multiple_of((j * CH + b) * 128, 128)
                    row = jnp.broadcast_to(wrow[ch : ch + 1, pl.ds(at, 128)], (16, 128))
                    after = pltpu.roll(row, 1 + 16 * g, 1, stride=1, stride_axis=0)
                    if b:
                        block = jnp.where(first, before, after).astype(BF16)
                        into[rows, (b - 1) * 128 : b * 128] = block
                        if b == 1 and ahead is not None:
                            ahead[rows, CH * 128 : (CH + 1) * 128] = block
                    before = after
                if new is not None:
                    new[rows, :] = before.astype(BF16)

    def multiply(j, held, tiles=CH // 2):
        for p in range(tiles):
            halves = []
            for ch in range(CHANS):
                for h in range(2):
                    at = (2 * p + h) * 128
                    halves.append(held[ch * TAPS : (ch + 1) * TAPS, at : at + 256])
            out = jnp.dot(
                amat[...], jnp.concatenate(halves, axis=0), preferred_element_type=F32)
            for g in range(NQ * NT // 8):
                for b in range(2):
                    part[pl.ds(g * 8 * NBLK + j * CH + 2 * p + b, 8, stride=NBLK), :] = out[
                        g * 8 : (g + 1) * 8, b * 128 : (b + 1) * 128
                    ]

    def chunks(i, _):
        multiply(3 * i, hank0)
        build(3 * i + 2, hank2, hank1, last1, last2)
        multiply(3 * i + 1, hank1)
        build(3 * i + 3, hank0, hank2, last2, last0)
        multiply(3 * i + 2, hank2)
        build(3 * i + 4, hank1, hank0, last0, last1)
        return 0

    build(0, hank0, None, None, last0)
    build(1, hank1, hank0, last0, last1)
    inputs[0].wait()
    inputs[2].wait()
    inputs[3].wait()

    total = jnp.zeros((NT, 128), F32)
    flip_i = lax.broadcasted_iota(jnp.int32, (128, 128), 0)
    flip_j = lax.broadcasted_iota(jnp.int32, (128, 128), 1)
    flip = jnp.where(flip_i + flip_j == 127, 1.0, 0.0).astype(BF16)
    for ch in range(CHANS):
        for k in range(LEN // TAPS):
            piece = temp_ref[:, ch * LEN + k * TAPS : ch * LEN + (k + 1) * TAPS]
            wide = piece.astype(F32)
            total = total + wide * wide
            turned = jnp.dot(piece, flip, preferred_element_type=F32).astype(BF16)
            at = (ch * 2 + k % 2) * TAPS
            amat[(k // 2) * NT : (k // 2 + 1) * NT, at : at + TAPS] = turned
    norm = jnp.sqrt(jnp.sum(total, axis=1, keepdims=True) + 1e-6)
    scl[...] = jnp.broadcast_to(1.0 / norm, (NT, 128))
    lax.fori_loop(0, 3, chunks, 0)
    multiply(9, hank0)
    build(11, hank2, hank1, last1, last2)
    multiply(10, hank1)
    build(12, hank0, hank2, last2)
    multiply(11, hank2)
    multiply(12, hank0, 1)

    lane24 = lax.broadcasted_iota(jnp.int32, (ROWS, 128), 1)

    def shifted(t):
        lag = lag_ref[0, t]
        here = pres_ref[0, t].astype(F32)
        a, r = lax.shift_right_logical(lag, 7), lax.bitwise_and(lag, 127)
        left = right = None
        for q in range(NQ):
            at = (q * NT + t) * NBLK + 2 * q + a
            one, two = part[pl.ds(at, ROWS), :], part[pl.ds(at + 1, ROWS), :]
            left = one if left is None else left + one
            right = two if right is None else right + two
        by = lax.bitwise_and(128 - r, 127)
        left, right = pltpu.roll(left, by, 1), pltpu.roll(right, by, 1)
        return jnp.where(lane24 < 128 - r, left, right) * (scl[pl.ds(t, 1), :] * here)

    def place(k):
        return (z + 4 + k // 2 - (k % 2) * k + 8) % 8

    beyond = [(z + AWAY[k]) % 8 for k in range(8)]
    others = [(x + d) % 4 for d in range(4)]
    group = [others[d] * 16 for d in range(4)]

    def copy_c(k):
        return pltpu.make_async_remote_copy(
            src_ref=sendc.at[k], dst_ref=recvc.at[k], send_sem=sem_cs, recv_sem=sem_cr.at[k],
            device_id=dev(x, z, 1 - c), device_id_type=MESH)

    def copy_x(k, d):
        return pltpu.make_async_remote_copy(
            src_ref=sendx.at[k, d - 1], dst_ref=recvx.at[k, d - 1],
            send_sem=sem_xs, recv_sem=sem_xr.at[k],
            device_id=dev(others[d], z, c), device_id_type=MESH)

    def copy_z(k):
        return pltpu.make_async_remote_copy(
            src_ref=sendz.at[k], dst_ref=recvz.at[k], send_sem=sem_zs, recv_sem=sem_zr,
            device_id=dev(x, beyond[k], c), device_id_type=MESH)

    def both(k):
        at = beyond[k] * 2
        for d in range(4):
            sendc[k, d] = shifted(group[d] + at + 1 - c)
        copy_c(k).start()
        for d in range(4):
            own[k, d] = shifted(group[d] + at + c)

    def fold(k):
        copy_c(k).wait_recv()
        for d in (2, 1, 3):
            sendx[k, d - 1] = own[k, d] + recvc[k, d]
            copy_x(k, d).start()

    def reduced(k):
        pltpu.make_async_copy(sendx.at[k], recvx.at[k], sem_xr.at[k]).wait()
        total = (own[k, 0] + recvc[k, 0]) + (recvx[k, 0] + recvx[k, 1] + recvx[k, 2])
        if k < 7:
            sendz[k] = total
            copy_z(k).start()
        return total

    pl.semaphore_wait(barrier, 1 + 3 + 7 + 7)
    for k in range(8):
        both(k)
        if k >= 5:
            fold(k - 5)
    for k in range(3, 8):
        fold(k)
    for k in range(7):
        reduced(k)
    row = reduced(7)
    pltpu.make_async_copy(sendz, recvz, sem_zr).wait()
    for k in range(7):
        row = row + recvz[k]

    pos = jnp.clip(jnp.abs(row) * (BINS / 512.0) - 0.5, 0.0, BINS - 1.0)
    low = jnp.minimum(jnp.floor(pos), BINS - 2.0)
    high = jnp.floor(low * (1.0 / 32.0))
    inside = pos - 32.0 * high
    iota_h = lax.broadcasted_iota(jnp.int32, (32, 128), 0).astype(F32)
    iota_l = lax.broadcasted_iota(jnp.int32, (40, 128), 0).astype(F32)
    ones, hats = [], [[], [], []]
    for i in range(ROWS):
        ones.append(jnp.where(iota_h == high[i : i + 1, :], 1.0, 0.0).astype(BF16))
        hat = jnp.maximum(1.0 - jnp.abs(inside[i : i + 1, :] - iota_l), 0.0)
        for k in range(3):
            near = hat.astype(BF16)
            hats[k].append(near)
            hat = hat - near.astype(F32)
    ones = jnp.concatenate(ones, axis=1)
    stacked = jnp.concatenate([jnp.concatenate(piece, axis=1) for piece in hats], axis=0)
    counts = lax.dot_general(stacked, ones, (((1,), (1,)), ((), ())), preferred_element_type=F32)
    counts = counts[0:40, :] + counts[40:80, :] + counts[80:120, :]
    over = jnp.concatenate([jnp.zeros((1, 1), F32), counts[32:33, 0:31]], axis=1)
    row_l = lax.broadcasted_iota(jnp.int32, (32, 32), 0)
    col_h = lax.broadcasted_iota(jnp.int32, (32, 32), 1)
    below = jnp.where(col_h < row_l, 1.0, 0.0)
    above = jnp.where(row_l < col_h, 1.0, 0.0)
    sums = jnp.broadcast_to(jnp.sum(counts, axis=0, keepdims=True), (8, 32))
    before = jnp.dot(
        below, counts[0:32, :], precision=lax.Precision.HIGHEST, preferred_element_type=F32)
    before = before + jnp.dot(
        sums, above, precision=lax.Precision.HIGHEST, preferred_element_type=F32)[0:1, :]
    over = jnp.where(row_l == 0, jnp.broadcast_to(over, (32, 32)), 0.0)
    before = before - over
    counts = counts[0:32, :] + over
    share = jnp.clip((0.5 * TOUT - before) / jnp.maximum(counts, 1.0), 0.0, 1.0)
    share = jnp.sum(jnp.sum(share, axis=0, keepdims=True), axis=1, keepdims=True)
    mad = 1.4826 * ((512.0 / BINS) * share)
    pk[0:ROWS] = row / mad
    madrow = jnp.broadcast_to(mad, (8, 128))

    lane8 = lax.broadcasted_iota(jnp.int32, (8, 128), 1)
    for j in range(8):
        at, off = (OWN * j) // 128, (OWN * j) % 128
        piece = pk[pl.ds(at, 8, stride=3), :]
        if off:
            piece = pltpu.roll(piece, 128 - off, 1)
            if off + OWN > 128:
                nxt = pltpu.roll(pk[pl.ds(at + 1, 8, stride=3), :], 128 - off, 1)
                piece = jnp.where(lane8 < 128 - off, piece, nxt)
        piece = jnp.where(lane8 < OWN, piece, madrow)
        for g in range(8):
            outr[8 * g + j] = piece[g : g + 1, :]

    def copy_o(xx, zz, cc):
        to = xx * 16 + zz * 2 + cc
        return pltpu.make_async_remote_copy(
            src_ref=outr.at[to], dst_ref=got.at[s], send_sem=sem_os, recv_sem=sem_or,
            device_id=(to, tp), device_id_type=MESH)

    def send(k, _):
        zz = place(k)
        for d in (2, 1, 3, 0):
            copy_o(others[d], zz, c).start()
            copy_o(others[d], zz, 1 - c).start()
        return 0

    lax.fori_loop(0, 7, send, 0)
    for d in (2, 1, 3):
        copy_o(others[d], z, c).start()
        copy_o(others[d], z, 1 - c).start()
    copy_o(x, z, 1 - c).start()
    got[s] = outr[s]
    pltpu.make_async_copy(outr.at[pl.ds(0, 63)], got.at[pl.ds(0, 63)], sem_or).wait()

    best = jnp.max(got[...], axis=0)
    pk1[...] = best

    def copy_p(d):
        return pltpu.make_async_remote_copy(
            src_ref=pk1, dst_ref=pkgot.at[d - 1], send_sem=sem_ps, recv_sem=sem_pr, device_id=(s, (tp + d) % 8), device_id_type=MESH)

    for d in (4, 3, 5, 2, 6, 1, 7):
        copy_p(d).start()
    flat = jnp.concatenate([got[i] for i in range(64)] + [jnp.zeros((64, 128), F32)], axis=0)
    turned = flat.T
    score_ref[...] = turned[0:OWN, 0:NT]
    mad_ref[...] = turned[OWN : OWN + 1, 0:NT]
    pltpu.make_async_copy(pkgot, pkgot, sem_pr).wait()
    for d in range(7):
        best = jnp.maximum(best, pkgot[d])
    peak_ref[...] = best[:, 0:OWN]

    pltpu.make_async_copy(sendc, recvc, sem_cs).wait()
    pltpu.make_async_copy(sendx, recvx, sem_xs).wait()
    pltpu.make_async_copy(sendz, recvz, sem_zs).wait()
    pltpu.make_async_copy(pkgot, pkgot, sem_ps).wait()
    pltpu.make_async_copy(outr.at[pl.ds(0, 63)], got.at[pl.ds(0, 63)], sem_os).wait()


def put_out(a, b, c, a_out, b_out, c_out, sems):
    copies = [
        pltpu.make_async_copy(one, two, sems.at[i])
        for i, (one, two) in enumerate(((a, a_out), (b, b_out), (c, c_out)))
    ]
    for copy in copies:
        copy.start()
    for copy in copies:
        copy.wait()


def on_device(waveform, templates, lags, present):
    vmem = pl.BlockSpec(memory_space=pltpu.VMEM)
    dma = pltpu.SemaphoreType.DMA
    hbm = pl.BlockSpec(memory_space=pltpu.HBM)
    results = pl.pallas_call(
        kernel,
        out_shape=(
            jax.ShapeDtypeStruct((OWN, NT), F32),
            jax.ShapeDtypeStruct((1, NT), F32),
            jax.ShapeDtypeStruct((1, OWN), F32),
        ),
        in_specs=[hbm, hbm, hbm, hbm],
        out_specs=(vmem, vmem, vmem),
        scratch_shapes=[
            pltpu.VMEM((CHANS, SAMPLES), BF16),
            pltpu.VMEM((NT, CHANS * LEN), BF16),
            pltpu.SMEM((1, NT), jnp.int32),
            pltpu.SMEM((1, NT), jnp.int32),
            dma((4,)),
            pltpu.VMEM((8, 53 * 128), F32),
            pltpu.VMEM((NQ * NT, 2 * CHANS * TAPS), BF16),
            pltpu.VMEM((CHANS * TAPS, (CH + 1) * 128), BF16),
            pltpu.VMEM((CHANS * TAPS, (CH + 1) * 128), BF16),
            pltpu.VMEM((CHANS * TAPS, (CH + 1) * 128), BF16),
            pltpu.VMEM((CHANS * TAPS, 128), BF16),
            pltpu.VMEM((CHANS * TAPS, 128), BF16),
            pltpu.VMEM((CHANS * TAPS, 128), BF16),
            pltpu.VMEM((NQ * NT * NBLK + 64, 128), F32),
            pltpu.VMEM((NT, 128), F32),
            pltpu.VMEM((8, 4, ROWS, 128), F32),
            pltpu.VMEM((8, 4, ROWS, 128), F32),
            pltpu.VMEM((8, 4, ROWS, 128), F32),
            pltpu.VMEM((8, 3, ROWS, 128), F32),
            pltpu.VMEM((8, 3, ROWS, 128), F32),
            pltpu.VMEM((7, ROWS, 128), F32),
            pltpu.VMEM((7, ROWS, 128), F32),
            pltpu.VMEM((64, 1, 128), F32),
            pltpu.VMEM((64, 1, 128), F32),
            pltpu.VMEM((ROWS + 8, 128), F32),
            pltpu.VMEM((1, 128), F32),
            pltpu.VMEM((7, 1, 128), F32),
            dma(()), dma((8,)), dma(()), dma((8,)), dma(()), dma(()),
            dma(()), dma(()), dma(()), dma(()),
        ],
        compiler_params=pltpu.CompilerParams(
            collective_id=0, has_side_effects=True, vmem_limit_bytes=50 * 1024 * 1024),
    )(
        *(
            pltpu.with_memory_space_constraint(value, pltpu.HBM)
            for value in (
                waveform[0], templates[:, 0, :], lags.reshape(1, NT), present.reshape(1, NT))
        )
    )
    score, mad, peak = pl.pallas_call(
        put_out,
        out_shape=(
            jax.ShapeDtypeStruct((OWN, NT), F32),
            jax.ShapeDtypeStruct((1, NT), F32),
            jax.ShapeDtypeStruct((1, OWN), F32),
        ),
        in_specs=[vmem, vmem, vmem],
        out_specs=(hbm, hbm, hbm),
        scratch_shapes=[dma((3,))],
        compiler_params=pltpu.CompilerParams(vmem_limit_bytes=1024 * 1024),
    )(*results)
    return score, mad[0], peak[0]


def solution(mesh):
    return jax.shard_map(
        on_device,
        mesh=mesh,
        in_specs=(P("sta", None, None), P("tpl", "sta", None), P("tpl", "sta"), P("tpl", "sta")),
        out_specs=(P("sta", "tpl"), P("tpl"), P("sta")),
        check_vma=False,
    )
```
